32 devices in a mesh: dp: 4 (over x, y), sp: 8 (over z, core).
Axes of the slice: x: 2, y: 2, z: 4, core: 2. Of those that a mesh axis runs over, the one named last changes fastest.
Arguments:
- x: bfloat16 [16384, 5376], P(('dp', 'sp')), parts along dimension 0
- gain: bfloat16 [5376], replicated
- wq: bfloat16 [5376, 4096], replicated
- wk: bfloat16 [5376, 2048], replicated
- wv: bfloat16 [5376, 2048], replicated
- wo: bfloat16 [4096, 5376], replicated
Outputs:
- output: bfloat16 [16384, 5376], P(('dp', 'sp')), parts along dimension 0
There are 4 independent parts. The reference program is written for one: setup_inputs(seed, part) draws one part's arguments, and reference() takes and returns one part's arrays. A program takes and returns all parts, laid end to end along the dimension named above; an argument that names none is the same for every part.
All inputs are finite; a program needn't handle non-finite values.
Results may differ from the reference program's by a relative error of at most 0.012.
Values are sent between devices in bfloat16 or wider.
A program may use at most 2 GiB of HBM per device.

```python
import jax
import jax.numpy as jnp
from jax import lax

ROWS = 4096
D = 5376
HEADS = 32
KV_HEADS = 16
HEAD = 128
THETA = 10000


def setup_inputs(seed: int = 0, part: int = 0) -> dict:
    kx, kn, kq, kk, kv, ko = jax.random.split(jax.random.key(seed), 6)

    def weights(key, rows, columns):
        return jax.random.normal(key, (rows, columns), jnp.float32) * rows**-0.5

    drawn = {
        "x": jax.random.normal(jax.random.fold_in(kx, part), (ROWS, D), jnp.float32),
        "gain": 1 + 0.1 * jax.random.normal(kn, (D,), jnp.float32),
        "wq": 2 * weights(kq, D, HEADS * HEAD),
        "wk": 2 * weights(kk, D, KV_HEADS * HEAD),
        "wv": 4 * weights(kv, D, KV_HEADS * HEAD),
        "wo": weights(ko, HEADS * HEAD, D),
    }
    return {k: v.astype(jnp.bfloat16) for k, v in drawn.items()}


def normed(x, gain):
    wide = x.astype(jnp.float32)
    scale = lax.rsqrt(jnp.mean(wide * wide, -1, keepdims=True) + 1e-6)
    return (wide * scale * gain.astype(jnp.float32)).astype(jnp.bfloat16)


def turned(t, place, theta):
    half = t.shape[-1] // 2
    angle = place.astype(jnp.float32)[:, None] * theta ** (-jnp.arange(half, dtype=jnp.float32) / half)
    cos, sin = jnp.cos(angle)[:, None], jnp.sin(angle)[:, None]
    a, b = t[..., :half].astype(jnp.float32), t[..., half:].astype(jnp.float32)
    return jnp.concatenate([a * cos - b * sin, b * cos + a * sin], -1).astype(jnp.bfloat16)


def matmul(a, w):
    return jnp.dot(a, w, preferred_element_type=jnp.float32).astype(jnp.bfloat16)


def einsum(form, a, b):
    return jnp.einsum(form, a.astype(jnp.float32), b.astype(jnp.float32))


def attention(q, k, v):
    scores = einsum("tgsd,ugd->gstu", q, k) * q.shape[-1] ** -0.5
    token = jnp.arange(q.shape[0])
    scores = jnp.where(token[:, None] >= token, scores, -jnp.inf)
    weights = jax.nn.softmax(scores, -1).astype(jnp.bfloat16)
    return einsum("gstu,ugd->tgsd", weights, v).astype(jnp.bfloat16)


def reference(x, gain, wq, wk, wv, wo):
    a, place = normed(x, gain), jnp.arange(ROWS)
    q = turned(matmul(a, wq).reshape(ROWS, HEADS, HEAD), place, THETA).reshape(ROWS, KV_HEADS, -1, HEAD)
    k = turned(matmul(a, wk).reshape(ROWS, KV_HEADS, HEAD), place, THETA)
    v = matmul(a, wv).reshape(ROWS, KV_HEADS, HEAD)
    seen = attention(q, k, v).reshape(ROWS, HEADS * HEAD)
    return (x.astype(jnp.float32) + jnp.dot(seen, wo, preferred_element_type=jnp.float32)).astype(jnp.bfloat16)
```

```python
import functools

import jax
import jax.numpy as jnp
from jax import lax
from jax.experimental import pallas as pl
from jax.experimental.pallas import tpu as pltpu
from jax.sharding import PartitionSpec as P

HEAD = 128
THETA = 10000
NEG = -1e30
HIDDEN = 2 * NEG
LOG2E = 1.4426950408889634
MESH = pl.DeviceIdType.MESH
COLS = 256
SLOTS = 3
VMEM = 67_043_328


def _dot(a, b, ca, cb):
    return lax.dot_general(a, b, (((ca,), (cb,)), ((), ())), preferred_element_type=jnp.float32)


def _kernel(rounds, chips, a_ref, cos_ref, sin_ref, wq_ref, wk_ref, wv_ref, out_ref, w_s, own, staged, kv_up, q_down, part, part_lse, lse_s,
            o_got, top_s, mix_s, gap_s, w_sem, dd_send, dd_recv, kv_send, kv_recv, kvf_send, kvf_recv, q_send, q_recv, p_send, p_recv,
            l_send, l_recv, o_send, o_recv, out_sem):
    me = lax.axis_index("sp")
    z, core = lax.div(me, 2), lax.rem(me, 2)
    other = 1 - core
    mate = 2 * z + other
    T = a_ref.shape[0]
    e = HEAD**-0.5 * LOG2E
    scale = HEAD**-0.5
    pieces = [(h, i, (2 * h + i) * T) for h in range(2) for i in range(2)]

    def copy(src, dst, send, recv, to):
        return pltpu.make_async_remote_copy(src_ref=src, dst_ref=dst, send_sem=send, recv_sem=recv, device_id={"sp": to}, device_id_type=MESH)

    def dd(ab, isq, j):
        return copy(staged.at[ab, isq, j], own.at[ab, isq, j, :, core], dd_send.at[ab, isq, j], dd_recv.at[ab, isq, j], mate)

    def kv_first(j, theirs):
        src = staged.at[0, 0, j] if theirs else own.at[0, 0, j, :, core]
        to = 2 * lax.min(z + 1, chips - 1) + (other if theirs else core)
        return copy(src, kv_up.at[0, j, :, core], kv_send.at[theirs, j], kv_recv.at[core, j], to)

    def kv_next(s, j):
        to = 2 * lax.min(z + 1, chips - 1) + core
        return copy(kv_up.at[s - 1, j], kv_up.at[s, j], kvf_send.at[s - 1, j], kvf_recv.at[s - 1, j], to)

    def q_to(d, j, theirs):
        src = staged.at[1, 1, j] if theirs else own.at[1, 1, j, :, core]
        to = 2 * lax.max(z - d, 0) + (other if theirs else core)
        return copy(src, q_down.at[d - 1, j, :, core], q_send.at[d - 1, theirs, j], q_recv.at[d - 1, core, j], to)

    def p_to(d, j):
        to = 2 * lax.min(z + 1, chips - 1) + core
        return copy(q_down.at[d - 1, j], part.at[d - 1, j], p_send.at[d - 1, j], p_recv.at[d - 1, j], to)

    def l_to(d, j):
        to = 2 * lax.min(z + 1, chips - 1) + core
        return copy(lse_s.at[d - 1, j], part_lse.at[d - 1, j], l_send.at[d - 1, j], l_recv.at[d - 1, j], to)

    def o_to(ab, j):
        return copy(own.at[ab, 1, j, :, other], o_got.at[ab, j], o_send.at[ab, j], o_recv.at[ab, j], mate)

    def kv_first_here(j, half):
        return copy(kv_up.at[0, j, :, half], kv_up.at[0, j, :, half], kv_send.at[0, j], kv_recv.at[half, j], mate)

    def kv_next_here(s, j):
        return copy(kv_up.at[s - 1, j], kv_up.at[s - 1, j], kvf_send.at[0, j], kvf_recv.at[s - 2, j], mate)

    def q_here(d, j, half):
        return copy(q_down.at[d - 1, j, :, half], q_down.at[d - 1, j, :, half], q_send.at[0, 0, j], q_recv.at[d - 1, half, j], mate)

    def p_here(d, j):
        return copy(part.at[d, j], part.at[d, j], p_send.at[0, j], p_recv.at[d, j], mate)

    def l_here(d, j):
        return copy(part_lse.at[d, j], part_lse.at[d, j], l_send.at[0, j], l_recv.at[d, j], mate)

    def weights(n):
        j, b = lax.div(n, 8), lax.rem(n, 8)
        pair, k = lax.div(b, 2), lax.rem(b, 2)
        ab = jnp.where((pair == 1) | (pair == 2), 1, 0)
        slot = lax.rem(n, SLOTS)
        at_kv = pl.ds(pl.multiple_of(COLS * (rounds * ab + j), COLS), COLS)
        at_q = pl.ds(pl.multiple_of(COLS * (2 * (rounds * ab + j) + k), COLS), COLS)
        isq = lax.rem(pair, 2)

        @pl.when((isq == 0) & (k == 0))
        def _():
            pltpu.make_async_copy(wk_ref.at[:, at_kv], w_s.at[slot], w_sem.at[slot]).start()

        @pl.when((isq == 0) & (k == 1))
        def _():
            pltpu.make_async_copy(wv_ref.at[:, at_kv], w_s.at[slot], w_sem.at[slot]).start()

        @pl.when(isq == 1)
        def _():
            pltpu.make_async_copy(wq_ref.at[:, at_q], w_s.at[slot], w_sem.at[slot]).start()

    def project(j):
        def block(b, _):
            n = 8 * j + b
            slot = lax.rem(n, SLOTS)

            @pl.when(n + SLOTS - 1 < 8 * rounds)
            def _():
                weights(n + SLOTS - 1)

            pltpu.make_async_copy(wk_ref.at[:, pl.ds(0, COLS)], w_s.at[slot], w_sem.at[slot]).wait()
            pair, k = lax.div(b, 2), lax.rem(b, 2)
            isq = lax.rem(pair, 2)
            ab = jnp.where((pair == 1) | (pair == 2), 1, 0)
            t = jnp.dot(a_ref[...], w_s[slot], preferred_element_type=jnp.float32).astype(jnp.bfloat16)
            turn = (isq == 1) | (k == 0)
            for u in range(2):
                plain = t[:, u * HEAD : (u + 1) * HEAD]
                f = plain.astype(jnp.float32)
                rotated = (f * cos_ref[...] + pltpu.roll(f, HEAD // 2, 1) * sin_ref[...]).astype(jnp.bfloat16)
                tile = jnp.where(turn, rotated, plain)
                owner = jnp.where(isq == 1, k, u)
                index = jnp.where(isq == 1, u, k)

                @pl.when(owner == core)
                def _():
                    own[ab, isq, j, index, core] = tile

                @pl.when(owner != core)
                def _():
                    staged[ab, isq, j, index] = tile

            @pl.when(k == 1)
            def _():
                dd(ab, isq, j).start()

            @pl.when((b == 1) & (z < chips - 1))
            def _():
                kv_first(j, 0).start()
                kv_first(j, 1).start()

            @pl.when(b == 3)
            def _():
                for d in range(chips - 1, 0, -1):

                    @pl.when(z >= d)
                    def _():
                        q_to(d, j, 0).start()
                        q_to(d, j, 1).start()

            return 0

        lax.fori_loop(0, 8, block, 0)

    def fresh():
        top_s[...] = jnp.full(top_s.shape, NEG, jnp.float32)
        mix_s[...] = jnp.zeros(mix_s.shape, jnp.float32)

    def carried(out, lse):
        top_s[...] = lse[...] * (1 / scale)
        for h, i, at in pieces:
            mix_s[:HEAD, at : at + T] = out[h, i].astype(jnp.float32).T
        mix_s[HEAD:, :] = jnp.ones((8, 4 * T), jnp.float32)

    def block(q, kv, b, which, masked):
        k, v = kv[0, b], kv[1, b]
        scores = [_dot(k, q[h, i], 1, 1) for h, i, _ in which]
        weights_, keeps = [], []
        for (h, i, at), s in zip(which, scores):
            if (h, i) in masked:
                s = jnp.where(gap_s[...] >= 0, s, HIDDEN)
            old = top_s[:, at : at + T]
            top = jnp.maximum(old, s.max(axis=0, keepdims=True))
            top_s[:, at : at + T] = top
            weights_.append(jnp.exp2((s - top) * e).astype(jnp.bfloat16))
            keeps.append(jnp.exp2((old - top) * e))
        values = jnp.concatenate([v.T, jnp.ones((8, T), jnp.bfloat16)], axis=0)
        for (h, i, at), p, keep in zip(which, weights_, keeps):
            mix_s[:, at : at + T] = mix_s[:, at : at + T] * keep + _dot(values, p, 1, 0)

    def whole(q, kv):
        lax.fori_loop(0, 2, lambda b, _: (block(q, kv, b, pieces, ()), 0)[1], 0)

    def diagonal(q, kv):
        block(q, kv, 0, pieces, ((0, 0), (1, 0)))
        block(q, kv, 1, [p for p in pieces if p[1] == 1], ((0, 1), (1, 1)))

    def finish(out, lse=None):
        for h, i, at in pieces:
            total = mix_s[HEAD : HEAD + 1, at : at + T]
            out[h, i] = (mix_s[:HEAD, at : at + T] * (1 / total)).T.astype(out.dtype)
            if lse is not None:
                lse[:, at : at + T] = top_s[:, at : at + T] * scale + jnp.log(total)

    def attend_a(j):
        dd(0, 0, j).wait_recv()
        dd(0, 1, j).wait_recv()
        fresh()
        diagonal(own.at[0, 1, j], own.at[0, 0, j])

        def from_below(s, _):
            @pl.when(s == 1)
            def _():
                kv_first_here(j, 0).wait_recv()
                kv_first_here(j, 1).wait_recv()

            @pl.when(s > 1)
            def _():
                kv_next_here(s, j).wait_recv()

            @pl.when(z < chips - 1)
            def _():
                kv_next(s, j).start()

            whole(own.at[0, 1, j], kv_up.at[s - 1, j])
            return 0

        lax.fori_loop(1, z + 1, from_below, 0)
        finish(own.at[0, 1, j])
        o_to(0, j).start()

    def attend_b(j):
        dd(1, 0, j).wait_recv()

        def for_above(n, _):
            d = chips - 1 - z - n
            q_here(d, j, 0).wait_recv()
            q_here(d, j, 1).wait_recv()

            @pl.when(z > 0)
            def _():
                p_here(d, j).wait_recv()
                l_here(d, j).wait_recv()
                carried(part.at[d, j], part_lse.at[d, j])

            @pl.when(z == 0)
            def _():
                fresh()

            whole(q_down.at[d - 1, j], own.at[1, 0, j])
            finish(q_down.at[d - 1, j], lse_s.at[d - 1, j])
            p_to(d, j).start()
            l_to(d, j).start()
            return 0

        lax.fori_loop(0, chips - 1 - z, for_above, 0)

    def attend_own_b(j):
        @pl.when(z == chips - 1)
        def _():
            dd(1, 0, j).wait_recv()

        dd(1, 1, j).wait_recv()

        @pl.when(z > 0)
        def _():
            p_here(0, j).wait_recv()
            l_here(0, j).wait_recv()
            carried(part.at[0, j], part_lse.at[0, j])

        @pl.when(z == 0)
        def _():
            fresh()

        diagonal(own.at[1, 1, j], own.at[1, 0, j])
        for d in range(1, chips):

            @pl.when(z >= d)
            def _():
                q_to(d, j, 0).wait_send()

        finish(own.at[1, 1, j])
        o_to(1, j).start()

    barrier = pltpu.get_barrier_semaphore()
    for n in range(1, 2 * chips):
        pl.semaphore_signal(barrier, inc=1, device_id={"sp": lax.rem(me + n, 2 * chips)}, device_id_type=MESH)
    for n in range(SLOTS - 1):
        weights(jnp.int32(n))
    gap_s[...] = lax.broadcasted_iota(jnp.int32, (T, T), 1) - lax.broadcasted_iota(jnp.int32, (T, T), 0)
    pl.semaphore_wait(barrier, 2 * chips - 1)

    late_b, late_own = lax.div(z, 2), lax.div(z + 1, 2)

    def step(n, _):
        @pl.when(n + 1 < rounds)
        def _():
            project(n + 1)

        @pl.when((n >= 0) & (n < rounds))
        def _():
            attend_a(n)

        jb = n - late_b

        @pl.when((z < chips - 1) & (jb >= 0) & (jb < rounds))
        def _():
            attend_b(jb)

        jo = n - late_own

        @pl.when((jo >= 0) & (jo < rounds))
        def _():
            attend_own_b(jo)

        return 0

    lax.fori_loop(-1, rounds + chips // 2, step, 0)

    def outs(ab, j):
        got = []
        for h in range(2):
            for n, (src, c) in enumerate(((own.at[ab, 1, j, h, core], core), (o_got.at[ab, j, h], other))):
                head = 4 * (rounds * ab + j) + 2 * c + h
                at = pl.ds(pl.multiple_of(head * HEAD, HEAD), HEAD)
                got.append(pltpu.make_async_copy(src, out_ref.at[:, at], out_sem.at[ab, j, 2 * h + n]))
        return got

    def last(j, _):
        for ab in range(2):
            o_to(ab, j).wait_recv()
            for c in outs(ab, j):
                c.start()
        return 0

    lax.fori_loop(0, rounds, last, 0)

    def drain(j, _):
        for ab in range(2):
            for c in outs(ab, j):
                c.wait()
            for isq in range(2):
                dd(ab, isq, j).wait_send()
            o_to(ab, j).wait_send()

        @pl.when(z < chips - 1)
        def _():
            kv_first(j, 0).wait_send()
            kv_first(j, 1).wait_send()

        for s in range(1, chips - 1):

            @pl.when((z < chips - 1) & (s <= z))
            def _():
                kv_next(s, j).wait_send()

        for d in range(1, chips):

            @pl.when(z >= d)
            def _():
                q_to(d, j, 1).wait_send()

            @pl.when(d <= chips - 1 - z)
            def _():
                p_to(d, j).wait_send()
                l_to(d, j).wait_send()

        return 0

    lax.fori_loop(0, rounds, drain, 0)


def attention(a, cos, sin, wq, wk, wv, group):
    T, chips = a.shape[0], group // 2
    rounds = wk.shape[1] // HEAD // 4
    low, wide = jnp.bfloat16, jnp.float32
    R, C = rounds, chips - 1
    dma = pltpu.SemaphoreType.DMA
    vmem, any_ = pl.BlockSpec(memory_space=pltpu.VMEM), pl.BlockSpec(memory_space=pl.ANY)
    return pl.pallas_call(
        functools.partial(_kernel, rounds, chips),
        out_shape=jax.ShapeDtypeStruct((T, wq.shape[1]), low),
        in_specs=[vmem, vmem, vmem, any_, any_, any_],
        out_specs=any_,
        scratch_shapes=[
            pltpu.VMEM((SLOTS, a.shape[1], COLS), low),
            pltpu.VMEM((2, 2, R, 2, 2, T, HEAD), low),
            pltpu.VMEM((2, 2, R, 2, T, HEAD), low),
            pltpu.VMEM((C, R, 2, 2, T, HEAD), low),
            pltpu.VMEM((C, R, 2, 2, T, HEAD), low),
            pltpu.VMEM((C, R, 2, 2, T, HEAD), low),
            pltpu.VMEM((C, R, 1, 4 * T), wide),
            pltpu.VMEM((C, R, 1, 4 * T), wide),
            pltpu.VMEM((2, R, 2, T, HEAD), low),
            pltpu.VMEM((1, 4 * T), wide),
            pltpu.VMEM((HEAD + 8, 4 * T), wide),
            pltpu.VMEM((T, T), jnp.int32),
            dma((SLOTS,)),
            dma((2, 2, R)), dma((2, 2, R)),
            dma((2, R)), dma((2, R)),
            dma((C, R)), dma((C, R)),
            dma((C, 2, R)), dma((C, 2, R)),
            dma((C, R)), dma((C, R)),
            dma((C, R)), dma((C, R)),
            dma((2, R)), dma((2, R)),
            dma((2, R, 4)),
        ],
        compiler_params=pltpu.CompilerParams(collective_id=0, has_side_effects=True, vmem_limit_bytes=VMEM),
        cost_estimate=pl.CostEstimate(flops=2 * T * a.shape[1] * 2 * wq.shape[1] + 8 * T * T * wq.shape[1], transcendentals=0,
                                      bytes_accessed=2 * (wq.size + wk.size + wv.size)),
    )(a, cos, sin, wq, wk, wv)


def normed(x, gain):
    wide = x.astype(jnp.float32)
    scale = lax.rsqrt(jnp.mean(wide * wide, -1, keepdims=True) + 1e-6)
    return (wide * scale * gain.astype(jnp.float32)).astype(jnp.bfloat16)


def angles(place):
    half = HEAD // 2
    angle = place.astype(jnp.float32)[:, None] * THETA ** (-jnp.arange(half, dtype=jnp.float32) / half)
    cos, sin = jnp.cos(angle), jnp.sin(angle)
    return jnp.concatenate([cos, cos], -1), jnp.concatenate([-sin, sin], -1)


def solution(mesh):
    group = mesh.shape["sp"]

    def step(x, gain, wq, wk, wv, wo):
        own = x.shape[0]
        first = lax.axis_index("sp") * own
        cos, sin = angles(first + jnp.arange(own))
        seen = attention(normed(x, gain), cos, sin, wq, wk, wv, group)
        y = jnp.dot(seen, wo, preferred_element_type=jnp.float32)
        return (x.astype(jnp.float32) + y).astype(jnp.bfloat16)

    tokens, whole = P(("dp", "sp"), None), P(None, None)
    return jax.shard_map(
        step,
        mesh=mesh,
        in_specs=(tokens, P(None), whole, whole, whole, whole),
        out_specs=tokens,
        check_vma=False,
    )
```

```python
import functools

import jax
import jax.numpy as jnp
from jax import lax
from jax.experimental import pallas as pl
from jax.experimental.pallas import tpu as pltpu
from jax.sharding import PartitionSpec as P

STEPS = 64
TASKS = (
    (3178512, 10522704, 1656329, 12591127, 212992, 2732039, 7401638, 16136499, 341303, 7915104, 6874663, 13653592, 2328288, 1381157, 1627688, 4765192, 6723128, 658038, 657930, 657930, 657930, 10,),
    (6307840, 5341216, 6483984, 7369120, 9482976, 461091, 6369410, 7615332, 2438562, 3686728, 12599888, 9569232, 1246532, 5531177, 8826901, 10885160, 1640562, 11942167, 4608600, 5666454, 3631143, 120,),
    (6303776, 4321280, 11563536, 13656512, 4457282, 6480017, 6562611, 1261649, 11621524, 1422418, 7411856, 8402292, 10527032, 7349668, 361601, 2689064, 6836263, 6702601, 7747847, 5642568, 1538103, 88,),
    (4223168, 4192, 10518768, 14733488, 9445456, 222243, 3179588, 7615396, 5559315, 1578388, 3519732, 2483256, 377896, 461064, 2566472, 3619176, 1513848, 658008, 657930, 657930, 657930, 10,),
)
PAIRS = (
    (10902564, 16650296, 47005,),
    (4360464, 13024687, 59189,),
    (5179848, 6403902, 23970,),
    (299475, 12053039, 50821,),
)
SUMS = (
    (7345527,),
    (16417436,),
    (12476569,),
    (12533913,),
)

PROJECT, KV_ON, Q_ON, A_OWN, A_BELOW, A_END, B_ABOVE, B_OWN, SUM, B_KEYS = range(10)

HEAD = 128
THETA = 10000
NEG = -1e30
HIDDEN = 2 * NEG
LOG2E = 1.4426950408889634
MESH = pl.DeviceIdType.MESH
COLS = 256
PARTS = 3
VMEM = 67_043_328


def _dot(a, b, ca, cb):
    return lax.dot_general(a, b, (((ca,), (cb,)), ((), ())), preferred_element_type=jnp.float32)


def _kernel(rounds, chips, x_ref, gain_ref, cos_ref, sin_ref, wq_ref, wk_ref, wv_ref, wo_ref, out_ref, a_s, w_s, wo_s, own, staged, pool,
            part, part_lse, lse_s, o_got, top_s, mix_s, y_s, x_sem, w_sem, wo_sem, dd_send, dd_recv, kv_send, kv_recv, kvf_send,
            kvf_recv, q_send, q_recv, qf_send, qf_recv, p_send, p_recv, l_send, l_recv, o_send, o_recv, out_sem):
    me = lax.axis_index("sp")
    z, core = lax.div(me, 2), lax.rem(me, 2)
    other = 1 - core
    mate = 2 * z + other
    above, below = lax.min(z + 1, chips - 1), lax.max(z - 1, 0)
    T, D = a_s.shape
    scale = HEAD**-0.5
    e = scale * LOG2E
    far = chips - 1
    pieces = [(h, i, (2 * h + i) * T) for h in range(2) for i in range(2)]

    def table(rows, per, bits):
        words = []
        for column in zip(*rows):
            w = jnp.int32(column[0])
            for c in range(1, chips):
                w = jnp.where(z == c, jnp.int32(column[c]), w)
            words.append(w)

        def entry(n):
            at = lax.div(n, per)
            w = words[0]
            for i in range(1, len(words)):
                w = jnp.where(at == i, words[i], w)
            return lax.shift_right_logical(w, bits * (n - per * at)) & (2**bits - 1)

        return entry

    task_at, pair_at, sum_at = table(TASKS, 3, 8), table(PAIRS, 6, 4), table(SUMS, 8, 3)

    def copy(src, dst, send, recv, to):
        return pltpu.make_async_remote_copy(src_ref=src, dst_ref=dst, send_sem=send, recv_sem=recv, device_id={"sp": to}, device_id_type=MESH)

    def dd(ab, isq, j):
        return copy(staged.at[ab, isq, j], own.at[ab, isq, j, :, core], dd_send.at[ab, isq, j], dd_recv.at[ab, isq, j], mate)

    def kv_first(j, theirs):
        src = staged.at[0, 0, j] if theirs else own.at[0, 0, j, :, core]
        return copy(src, pool.at[0, j, :, core], kv_send.at[theirs, j], kv_recv.at[core, j], 2 * above + (other if theirs else core))

    def kv_next(s, j):
        return copy(pool.at[s - 1, j], pool.at[s, j], kvf_send.at[s - 1, j], kvf_recv.at[s - 1, j], 2 * above + core)

    def q_first(j, theirs):
        src = staged.at[1, 1, j] if theirs else own.at[1, 1, j, :, core]
        return copy(src, pool.at[far - 1, j, :, core], q_send.at[theirs, j], q_recv.at[core, j], 2 * below + (other if theirs else core))

    def q_next(d, j):
        return copy(pool.at[far - d, j], pool.at[far - d - 1, j], qf_send.at[d - 1, j], qf_recv.at[d - 1, j], 2 * below + core)

    def held(d):
        return jnp.where(z > 0, d, d - 1)

    def p_to(d, j):
        return copy(part.at[held(d), j], part.at[d - 1, j], p_send.at[d - 1, j], p_recv.at[d - 1, j], 2 * above + core)

    def l_to(d, j):
        return copy(lse_s.at[d - 1, j], part_lse.at[d - 1, j], l_send.at[d - 1, j], l_recv.at[d - 1, j], 2 * above + core)

    def o_to(ab, j):
        return copy(own.at[ab, 1, j, :, other], o_got.at[ab, j], o_send.at[ab, j], o_recv.at[ab, j], mate)

    def arrived(ref, sem):
        copy(ref, ref, sem, sem, mate).wait_recv()

    def kv_arrived(s, j):
        @pl.when(s == 1)
        def _():
            for half in range(2):
                arrived(pool.at[0, j, :, half], kv_recv.at[half, j])

        @pl.when(s > 1)
        def _():
            arrived(pool.at[s - 1, j], kvf_recv.at[s - 2, j])

    def q_arrived(d, j):
        @pl.when(d == 1)
        def _():
            for half in range(2):
                arrived(pool.at[far - 1, j, :, half], q_recv.at[half, j])

        @pl.when(d > 1)
        def _():
            arrived(pool.at[far - d, j], qf_recv.at[d - 2, j])

    def p_arrived(d, j):
        arrived(part.at[d, j], p_recv.at[d, j])
        arrived(part_lse.at[d, j], l_recv.at[d, j])

    def weights(n):
        code = pair_at(lax.div(n, 2))
        j, pair, k = lax.div(code, 4), lax.rem(code, 4), lax.rem(n, 2)
        ab = jnp.where((pair == 1) | (pair == 2), 1, 0)
        at_kv = pl.ds(pl.multiple_of(COLS * (rounds * ab + j), COLS), COLS)
        at_q = pl.ds(pl.multiple_of(COLS * (2 * (rounds * ab + j) + k), COLS), COLS)
        isq = lax.rem(pair, 2)
        slot = lax.rem(n, 2)

        @pl.when((isq == 0) & (k == 0))
        def _():
            pltpu.make_async_copy(wk_ref.at[:, at_kv], w_s.at[slot], w_sem.at[slot]).start()

        @pl.when((isq == 0) & (k == 1))
        def _():
            pltpu.make_async_copy(wv_ref.at[:, at_kv], w_s.at[slot], w_sem.at[slot]).start()

        @pl.when(isq == 1)
        def _():
            pltpu.make_async_copy(wq_ref.at[:, at_q], w_s.at[slot], w_sem.at[slot]).start()

    def project(j, pair, done):
        isq = lax.rem(pair, 2)
        ab = jnp.where((pair == 1) | (pair == 2), 1, 0)

        def block(k, _):
            n = 2 * done + k
            slot = lax.rem(n, 2)

            @pl.when(n + 1 < 8 * rounds)
            def _():
                weights(n + 1)

            pltpu.make_async_copy(wk_ref.at[:, pl.ds(0, COLS)], w_s.at[slot], w_sem.at[slot]).wait()
            t = jnp.dot(a_s[...], w_s[slot], preferred_element_type=jnp.float32).astype(jnp.bfloat16)
            turn = (isq == 1) | (k == 0)
            for u in range(2):
                plain = t[:, u * HEAD : (u + 1) * HEAD]
                f = plain.astype(jnp.float32)
                rotated = (f * cos_ref[...] + pltpu.roll(f, HEAD // 2, 1) * sin_ref[...]).astype(jnp.bfloat16)
                tile = jnp.where(turn, rotated, plain)
                owner = jnp.where(isq == 1, k, u)
                index = jnp.where(isq == 1, u, k)

                @pl.when(owner == core)
                def _():
                    own[ab, isq, j, index, core] = tile

                @pl.when(owner != core)
                def _():
                    staged[ab, isq, j, index] = tile

            return 0

        lax.fori_loop(0, 2, block, 0)

        @pl.when((pair == 0) & (z < far))
        def _():
            kv_first(j, 0).start()
            kv_first(j, 1).start()

        @pl.when((pair == 1) & (z > 0))
        def _():
            q_first(j, 0).start()
            q_first(j, 1).start()

        dd(ab, isq, j).start()

        @pl.when(done == 4 * rounds - 1)
        def _():
            pltpu.make_async_copy(x_ref, a_s, x_sem.at[0]).start()

    def wo_block(n):
        code = sum_at(lax.div(n, PARTS))
        rows = pl.ds(pl.multiple_of(4 * HEAD * code, 4 * HEAD), 4 * HEAD)
        c = lax.rem(n, PARTS)
        width = D // PARTS
        slot = lax.rem(n, 2)
        return pltpu.make_async_copy(wo_ref.at[rows, pl.ds(pl.multiple_of(c * width, width), width)], wo_s.at[slot], wo_sem.at[slot])

    def output(j, ab, done):
        o_to(ab, j).wait_recv()

        def block(c, _):
            n = PARTS * done + c

            @pl.when(n + 1 < PARTS * 2 * rounds)
            def _():
                wo_block(n + 1).start()

            wo_block(n).wait()
            slot = lax.rem(n, 2)
            mine = jnp.concatenate([own[ab, 1, j, 0, core], own[ab, 1, j, 1, core]], axis=1)
            theirs = jnp.concatenate([o_got[ab, j, 0], o_got[ab, j, 1]], axis=1)
            rows = lambda c_: pl.ds(pl.multiple_of(2 * HEAD * c_, 2 * HEAD), 2 * HEAD)
            y_s[c] += _dot(mine, wo_s[slot, rows(core)], 1, 0) + _dot(theirs, wo_s[slot, rows(other)], 1, 0)
            return 0

        lax.fori_loop(0, PARTS, block, 0)

    def fresh(st):
        top_s[st] = jnp.full(top_s.shape[1:], NEG, jnp.float32)
        mix_s[st] = jnp.zeros(mix_s.shape[1:], jnp.float32)

    def carried(st, out, lse):
        top_s[st] = lse[...] * (1 / scale)
        for h, i, at in pieces:
            mix_s[st, :HEAD, at : at + T] = out[h, i].astype(jnp.float32).T
        mix_s[st, HEAD:, :] = jnp.ones((8, 4 * T), jnp.float32)

    def block(st, q, kv, b, which, masked):
        k, v = kv[0, b], kv[1, b]
        scores = [_dot(k, q[h, i], 1, 1) for h, i, _ in which]
        if masked:
            seen = lax.broadcasted_iota(jnp.int32, (T, T), 1) >= lax.broadcasted_iota(jnp.int32, (T, T), 0)
        weights_, keeps = [], []
        for (h, i, at), s in zip(which, scores):
            if (h, i) in masked:
                s = jnp.where(seen, s, HIDDEN)
            old = top_s[st, :, at : at + T]
            top = jnp.maximum(old, s.max(axis=0, keepdims=True))
            top_s[st, :, at : at + T] = top
            weights_.append(jnp.exp2((s - top) * e).astype(jnp.bfloat16))
            keeps.append(jnp.exp2((old - top) * e))
        values = jnp.concatenate([v.T, jnp.ones((8, T), jnp.bfloat16)], axis=0)
        for (h, i, at), p, keep in zip(which, weights_, keeps):
            mix_s[st, :, at : at + T] = mix_s[st, :, at : at + T] * keep + _dot(values, p, 1, 0)

    def whole(st, q, kv):
        lax.fori_loop(0, 2, lambda b, _: (block(st, q, kv, b, pieces, ()), 0)[1], 0)

    def diagonal(st, q, kv):
        block(st, q, kv, 0, pieces, ((0, 0), (1, 0)))
        block(st, q, kv, 1, [p for p in pieces if p[1] == 1], ((0, 1), (1, 1)))

    def finish(st, out, lse=None):
        for h, i, at in pieces:
            total = mix_s[st, HEAD : HEAD + 1, at : at + T]
            out[h, i] = (mix_s[st, :HEAD, at : at + T] * (1 / total)).T.astype(out.dtype)
            if lse is not None:
                lse[:, at : at + T] = top_s[st, :, at : at + T] * scale + jnp.log(total)

    spare = rounds

    def start_b(d, j):
        @pl.when(z > 0)
        def _():
            p_arrived(d, j)
            carried(spare, part.at[d, j], part_lse.at[d, j])

        @pl.when(z == 0)
        def _():
            fresh(spare)

    barrier = pltpu.get_barrier_semaphore()
    for n in range(1, 2 * chips):
        pl.semaphore_signal(barrier, inc=1, device_id={"sp": lax.rem(me + n, 2 * chips)}, device_id_type=MESH)
    cuts = x_sem.shape[0]
    height = T // cuts

    def x_cut(i):
        rows = pl.ds(pl.multiple_of(i * height, height), height)
        return pltpu.make_async_copy(x_ref.at[rows], a_s.at[rows], x_sem.at[i])

    for i in range(cuts):
        x_cut(i).start()
    weights(jnp.int32(0))
    wo_block(jnp.int32(0)).start()
    y_s[...] = jnp.zeros(y_s.shape, jnp.float32)
    group = 32
    tiles = [slice(c, c + HEAD) for c in range(0, D, HEAD)]

    def norm(i, _):
        x_cut(i).wait()

        def rows_(g, _):
            rows = pl.ds(pl.multiple_of(i * height + g * group, group), group)
            squares = jnp.zeros((group, HEAD), jnp.float32)
            for t in tiles:
                wide = a_s[rows, t].astype(jnp.float32)
                squares += wide * wide
            by = lax.rsqrt(squares.sum(axis=1, keepdims=True) / D + 1e-6)
            for t in tiles:
                a_s[rows, t] = (a_s[rows, t].astype(jnp.float32) * by * gain_ref[:, t].astype(jnp.float32)).astype(jnp.bfloat16)
            return 0

        return lax.fori_loop(0, height // group, rows_, 0)

    lax.fori_loop(0, cuts, norm, 0)
    pl.semaphore_wait(barrier, 2 * chips - 1)

    def step(n, counts):
        projected, summed = counts
        code = task_at(n)
        kind, j, which = code & 15, lax.shift_right_logical(code, 4) & 3, lax.shift_right_logical(code, 6)

        @pl.when(kind == PROJECT)
        def _():
            project(j, which, projected)

        @pl.when(kind == KV_ON)
        def _():
            kv_arrived(which, j)
            kv_next(which, j).start()

        @pl.when(kind == Q_ON)
        def _():
            q_arrived(which, j)
            q_next(which, j).start()

        @pl.when(kind == A_OWN)
        def _():
            dd(0, 0, j).wait_recv()
            dd(0, 1, j).wait_recv()
            fresh(j)
            diagonal(j, own.at[0, 1, j], own.at[0, 0, j])

        @pl.when(kind == A_BELOW)
        def _():
            @pl.when(z == far)
            def _():
                kv_arrived(which, j)

            whole(j, own.at[0, 1, j], pool.at[which - 1, j])

        @pl.when(kind == A_END)
        def _():
            finish(j, own.at[0, 1, j])
            o_to(0, j).start()

        @pl.when(kind == B_KEYS)
        def _():
            dd(1, 0, j).wait_recv()

        @pl.when(kind == B_ABOVE)
        def _():
            @pl.when(z == 0)
            def _():
                q_arrived(which, j)

            start_b(which, j)
            whole(spare, pool.at[far - which, j], own.at[1, 0, j])
            finish(spare, part.at[held(which), j], lse_s.at[which - 1, j])
            p_to(which, j).start()
            l_to(which, j).start()

        @pl.when(kind == B_OWN)
        def _():
            dd(1, 1, j).wait_recv()
            start_b(0, j)
            diagonal(spare, own.at[1, 1, j], own.at[1, 0, j])

            @pl.when(z > 0)
            def _():
                q_first(j, 0).wait_send()

            finish(spare, own.at[1, 1, j])
            o_to(1, j).start()

        @pl.when(kind == SUM)
        def _():
            output(j, which, summed)

        return projected + jnp.where(kind == PROJECT, 1, 0), summed + jnp.where(kind == SUM, 1, 0)

    lax.fori_loop(0, STEPS, step, (jnp.int32(0), jnp.int32(0)))

    pltpu.make_async_copy(x_ref, a_s, x_sem.at[0]).wait()
    width = D // PARTS

    def result(c):
        cols = pl.ds(c * width, width)
        return pltpu.make_async_copy(a_s.at[:, cols], out_ref.at[:, cols], out_sem.at[c])

    for c in range(PARTS):
        cols = slice(c * width, (c + 1) * width)
        for r in range(0, T, 32):
            a_s[r : r + 32, cols] = (a_s[r : r + 32, cols].astype(jnp.float32) + y_s[c, r : r + 32]).astype(jnp.bfloat16)
        result(c).start()

    def drain(j, _):
        for ab in range(2):
            for isq in range(2):
                dd(ab, isq, j).wait_send()
            o_to(ab, j).wait_send()

        @pl.when(z < far)
        def _():
            kv_first(j, 0).wait_send()
            kv_first(j, 1).wait_send()

        @pl.when(z > 0)
        def _():
            q_first(j, 1).wait_send()

        for s in range(1, far):

            @pl.when((z < far) & (s <= z))
            def _():
                kv_next(s, j).wait_send()

        for d in range(1, far):

            @pl.when((z > 0) & (d <= far - z))
            def _():
                q_next(d, j).wait_send()

        for d in range(1, chips):

            @pl.when(d <= far - z)
            def _():
                p_to(d, j).wait_send()
                l_to(d, j).wait_send()

        return 0

    lax.fori_loop(0, rounds, drain, 0)
    for c in range(PARTS):
        result(c).wait()


def layer(x, gain, cos, sin, wq, wk, wv, wo, group):
    T, D, chips = *x.shape, group // 2
    rounds = wk.shape[1] // HEAD // 4
    low, wide = jnp.bfloat16, jnp.float32
    R, C = rounds, chips - 1
    dma = pltpu.SemaphoreType.DMA
    vmem, any_ = pl.BlockSpec(memory_space=pltpu.VMEM), pl.BlockSpec(memory_space=pl.ANY)
    weights = wq.size + wk.size + wv.size + wo.size
    return pl.pallas_call(
        functools.partial(_kernel, rounds, chips),
        out_shape=jax.ShapeDtypeStruct((T, D), low),
        in_specs=[any_, vmem, vmem, vmem, any_, any_, any_, any_],
        out_specs=any_,
        scratch_shapes=[
            pltpu.VMEM((T, D), low),
            pltpu.VMEM((2, D, COLS), low),
            pltpu.VMEM((2, 4 * HEAD, D // PARTS), low),
            pltpu.VMEM((2, 2, R, 2, 2, T, HEAD), low),
            pltpu.VMEM((2, 2, R, 2, T, HEAD), low),
            pltpu.VMEM((C, R, 2, 2, T, HEAD), low),
            pltpu.VMEM((C, R, 2, 2, T, HEAD), low),
            pltpu.VMEM((C, R, 1, 4 * T), wide),
            pltpu.VMEM((C, R, 1, 4 * T), wide),
            pltpu.VMEM((2, R, 2, T, HEAD), low),
            pltpu.VMEM((R + 1, 1, 4 * T), wide),
            pltpu.VMEM((R + 1, HEAD + 8, 4 * T), wide),
            pltpu.VMEM((PARTS, T, D // PARTS), wide),
            dma((4,)), dma((2,)), dma((2,)),
            dma((2, 2, R)), dma((2, 2, R)),
            dma((2, R)), dma((2, R)),
            dma((C - 1, R)), dma((C - 1, R)),
            dma((2, R)), dma((2, R)),
            dma((C - 1, R)), dma((C - 1, R)),
            dma((C, R)), dma((C, R)),
            dma((C, R)), dma((C, R)),
            dma((2, R)), dma((2, R)),
            dma((PARTS,)),
        ],
        compiler_params=pltpu.CompilerParams(collective_id=0, has_side_effects=True, vmem_limit_bytes=VMEM),
        cost_estimate=pl.CostEstimate(flops=2 * T * weights + 8 * T * T * wq.shape[1], transcendentals=0, bytes_accessed=2 * weights),
    )(x, gain.reshape(1, D), cos, sin, wq, wk, wv, wo)


def angles(place):
    half = HEAD // 2
    angle = place.astype(jnp.float32)[:, None] * THETA ** (-jnp.arange(half, dtype=jnp.float32) / half)
    cos, sin = jnp.cos(angle), jnp.sin(angle)
    return jnp.concatenate([cos, cos], -1), jnp.concatenate([-sin, sin], -1)


def solution(mesh):
    group = mesh.shape["sp"]

    def step(x, gain, wq, wk, wv, wo):
        own = x.shape[0]
        cos, sin = angles(lax.axis_index("sp") * own + jnp.arange(own))
        return layer(x, gain, cos, sin, wq, wk, wv, wo, group)

    tokens, whole = P(("dp", "sp"), None), P(None, None)
    return jax.shard_map(
        step,
        mesh=mesh,
        in_specs=(tokens, P(None), whole, whole, whole, whole),
        out_specs=tokens,
        check_vma=False,
    )
```

```python
import functools

import jax
import jax.numpy as jnp
import numpy as np
from jax import lax
from jax.experimental import pallas as pl
from jax.experimental.pallas import tpu as pltpu
from jax.sharding import PartitionSpec as P

STEPS = 64
TASKS = (
    (8396816, 9449552, 1513968, 13619, 12600841, 2709664, 13021350, 14039104, 4719367, 381078, 6686950, 3740947, 14686454, 2433926, 3614832, 7889078, 2586198, 658024, 657930, 657930, 657930, 10,),
    (11550720, 6312208, 6475824, 14712929, 5538323, 15736945, 9584931, 3351908, 7607744, 1586514, 9478712, 2687904, 4502118, 361993, 4363801, 5646344, 5244786, 7382600, 3762215, 7751350, 3627031, 120,),
    (6299648, 3162384, 14697200, 2306897, 11555472, 5283985, 7454818, 7471988, 10567748, 1274064, 11818161, 3707957, 1401953, 1582500, 8661121, 557061, 599849, 1665094, 5773142, 7747942, 3622919, 120,),
    (11550928, 12603616, 7376992, 15732736, 10518547, 204884, 6562628, 3179668, 3347924, 11826200, 3536100, 2466872, 377896, 461064, 1513800, 2566488, 3619176, 658040, 657930, 657930, 657930, 10,),
)
PAIRS = (
    (7099012, 2007823, 40375,),
    (13192720, 4164391, 54694,),
    (16533888, 3518059, 11633,),
    (3522071, 15994217, 51362,),
)
SUMS = (
    (14487837,),
    (16204825,),
    (15917195,),
    (16433305,),
)

PROJECT, KV_ON, Q_ON, A_OWN, A_BELOW, A_END, B_ABOVE, B_OWN, SUM, B_KEYS = range(10)

HEAD = 128
THETA = 10000
NEG = -1e30
HIDDEN = 2 * NEG
LOG2E = 1.4426950408889634
MESH = pl.DeviceIdType.MESH
COLS = 256
PARTS = 3
WO_SLOTS = 4
VMEM = 61_440_000


def _dot(a, b, ca, cb):
    return lax.dot_general(a, b, (((ca,), (cb,)), ((), ())), preferred_element_type=jnp.float32)


def _kernel(rounds, chips, x_ref, gain_ref, speed_ref, turn_ref, wq_ref, wk_ref, wv_ref, wo_ref, a_s, turn_s, w_s, wo_s, seen_s, own, staged, pool,
            part, part_lse, lse_s, o_got, top_s, mix_s, y_s, x_sem, turn_sem, w_sem, wo_sem, dd_send, dd_recv, kv_send, kv_recv, kvf_send,
            kvf_recv, q_send, q_recv, qf_send, qf_recv, p_send, p_recv, l_send, l_recv, o_send, o_recv):
    me = lax.axis_index("sp")
    z, core = lax.div(me, 2), lax.rem(me, 2)
    other = 1 - core
    mate = 2 * z + other
    above, below = lax.min(z + 1, chips - 1), lax.max(z - 1, 0)
    T, D = a_s.shape
    scale = HEAD**-0.5
    e = scale * LOG2E
    far = chips - 1
    pieces = [(h, i, (2 * h + i) * T) for h in range(2) for i in range(2)]

    def table(rows, per, bits):
        words = []
        for column in zip(*rows):
            w = jnp.int32(column[0])
            for c in range(1, chips):
                w = jnp.where(z == c, jnp.int32(column[c]), w)
            words.append(w)

        def entry(n):
            at = lax.div(n, per)
            w = words[0]
            for i in range(1, len(words)):
                w = jnp.where(at == i, words[i], w)
            return lax.shift_right_logical(w, bits * (n - per * at)) & (2**bits - 1)

        return entry

    task_at, pair_at, sum_at = table(TASKS, 3, 8), table(PAIRS, 6, 4), table(SUMS, 8, 3)

    def copy(src, dst, send, recv, to):
        return pltpu.make_async_remote_copy(src_ref=src, dst_ref=dst, send_sem=send, recv_sem=recv, device_id={"sp": to}, device_id_type=MESH)

    def dd(ab, isq, j):
        return copy(staged.at[ab, isq, j], own.at[ab, isq, j, :, core], dd_send.at[ab, isq, j], dd_recv.at[ab, isq, j], mate)

    def kv_first(j, k, theirs):
        src = staged.at[0, 0, j, k] if theirs else own.at[0, 0, j, k, core]
        to = 2 * above + (other if theirs else core)
        return copy(src, pool.at[0, j, k, core], kv_send.at[theirs, k, j], kv_recv.at[core, k, j], to)

    def kv_next(s, j):
        return copy(pool.at[s - 1, j], pool.at[s, j], kvf_send.at[s - 1, j], kvf_recv.at[s - 1, j], 2 * above + core)

    def q_first(j, theirs):
        src = staged.at[1, 1, j] if theirs else own.at[1, 1, j, :, core]
        return copy(src, pool.at[far - 1, j, :, core], q_send.at[theirs, j], q_recv.at[core, j], 2 * below + (other if theirs else core))

    def q_next(d, j):
        return copy(pool.at[far - d, j], pool.at[far - d - 1, j], qf_send.at[d - 1, j], qf_recv.at[d - 1, j], 2 * below + core)

    def held(d):
        return jnp.where(z > 0, d, d - 1)

    def p_to(d, j):
        return copy(part.at[held(d), j], part.at[d - 1, j], p_send.at[d - 1, j], p_recv.at[d - 1, j], 2 * above + core)

    def l_to(d, j):
        return copy(lse_s.at[d - 1, j], part_lse.at[d - 1, j], l_send.at[d - 1, j], l_recv.at[d - 1, j], 2 * above + core)

    def o_to(ab, j):
        return copy(own.at[ab, 1, j, :, other], o_got.at[ab, j], o_send.at[ab, j], o_recv.at[ab, j], mate)

    def arrived(ref, sem):
        copy(ref, ref, sem, sem, mate).wait_recv()

    def kv_arrived(s, j):
        @pl.when(s == 1)
        def _():
            for half in range(2):
                for k in range(2):
                    arrived(pool.at[0, j, k, half], kv_recv.at[half, k, j])

        @pl.when(s > 1)
        def _():
            arrived(pool.at[s - 1, j], kvf_recv.at[s - 2, j])

    def q_arrived(d, j):
        @pl.when(d == 1)
        def _():
            for half in range(2):
                arrived(pool.at[far - 1, j, :, half], q_recv.at[half, j])

        @pl.when(d > 1)
        def _():
            arrived(pool.at[far - d, j], qf_recv.at[d - 2, j])

    def p_arrived(d, j):
        arrived(part.at[d, j], p_recv.at[d, j])
        arrived(part_lse.at[d, j], l_recv.at[d, j])

    def weights(n):
        code = pair_at(lax.div(n, 2))
        j, pair, k = lax.div(code, 4), lax.rem(code, 4), lax.rem(n, 2)
        ab = jnp.where((pair == 1) | (pair == 2), 1, 0)
        at_kv = pl.ds(pl.multiple_of(COLS * (rounds * ab + j), COLS), COLS)
        at_q = pl.ds(pl.multiple_of(COLS * (2 * (rounds * ab + j) + k), COLS), COLS)
        isq = lax.rem(pair, 2)
        slot = lax.rem(n, 2)

        @pl.when((isq == 0) & (k == 0))
        def _():
            pltpu.make_async_copy(wk_ref.at[:, at_kv], w_s.at[slot], w_sem.at[slot]).start()

        @pl.when((isq == 0) & (k == 1))
        def _():
            pltpu.make_async_copy(wv_ref.at[:, at_kv], w_s.at[slot], w_sem.at[slot]).start()

        @pl.when(isq == 1)
        def _():
            pltpu.make_async_copy(wq_ref.at[:, at_q], w_s.at[slot], w_sem.at[slot]).start()

    def project(j, pair, done):
        isq = lax.rem(pair, 2)
        ab = jnp.where((pair == 1) | (pair == 2), 1, 0)

        def block(k, _):
            n = 2 * done + k
            slot = lax.rem(n, 2)

            @pl.when(n + 1 < 8 * rounds)
            def _():
                weights(n + 1)

            pltpu.make_async_copy(wk_ref.at[:, pl.ds(0, COLS)], w_s.at[slot], w_sem.at[slot]).wait()
            t = jnp.dot(a_s[...], w_s[slot], preferred_element_type=jnp.float32).astype(jnp.bfloat16)
            turn = (isq == 1) | (k == 0)
            for u in range(2):
                plain = t[:, u * HEAD : (u + 1) * HEAD]
                f = plain.astype(jnp.float32)
                rotated = (f * turn_s[0] + pltpu.roll(f, HEAD // 2, 1) * turn_s[1]).astype(jnp.bfloat16)
                tile = jnp.where(turn, rotated, plain)
                owner = jnp.where(isq == 1, k, u)
                index = jnp.where(isq == 1, u, k)

                @pl.when(owner == core)
                def _():
                    own[ab, isq, j, index, core] = tile

                @pl.when(owner != core)
                def _():
                    staged[ab, isq, j, index] = tile

            @pl.when((pair == 0) & (z < far))
            def _():
                kv_first(j, k, 0).start()
                kv_first(j, k, 1).start()

            return 0

        lax.fori_loop(0, 2, block, 0)

        @pl.when((pair == 1) & (z > 0))
        def _():
            q_first(j, 0).start()
            q_first(j, 1).start()

        dd(ab, isq, j).start()

        @pl.when(done == 4 * rounds - 1)
        def _():
            pltpu.make_async_copy(x_ref, a_s, x_sem.at[0]).start()

    def wo_block(n):
        code = sum_at(lax.div(n, 2 * PARTS))
        c, theirs = lax.rem(n, PARTS), lax.rem(lax.div(n, PARTS), 2)
        who = jnp.where(theirs == 1, other, core)
        rows = pl.ds(pl.multiple_of(2 * HEAD * (2 * code + who), 2 * HEAD), 2 * HEAD)
        width = D // PARTS
        slot = lax.rem(n, WO_SLOTS)
        return pltpu.make_async_copy(wo_ref.at[rows, pl.ds(pl.multiple_of(c * width, width), width)], wo_s.at[slot], wo_sem.at[slot])

    def output(j, ab, done):
        width = D // PARTS
        last = done == 2 * rounds - 1

        @pl.when(done == 2 * rounds - 2)
        def _():
            pltpu.make_async_copy(x_ref, a_s, x_sem.at[0]).wait()

        seen_s[0] = jnp.concatenate([own[ab, 1, j, 0, core], own[ab, 1, j, 1, core]], axis=1)

        def block(h, _):
            n = 2 * PARTS * done + h
            c, theirs, slot = lax.rem(h, PARTS), lax.div(h, PARTS), lax.rem(n, WO_SLOTS)
            cols = pl.ds(pl.multiple_of(c * width, width), width)

            @pl.when(n + WO_SLOTS - 1 < 2 * PARTS * 2 * rounds)
            def _():
                wo_block(n + WO_SLOTS - 1).start()

            @pl.when(h == PARTS)
            def _():
                o_to(ab, j).wait_recv()
                seen_s[1] = jnp.concatenate([o_got[ab, j, 0], o_got[ab, j, 1]], axis=1)

            @pl.when((done == 0) & (theirs == 0))
            def _():
                y_s[c] = jnp.zeros(y_s.shape[1:], jnp.float32)

            @pl.when((done == 2 * rounds - 2) & (theirs == 0))
            def _():
                for r in range(0, T, 32):
                    y_s[c, r : r + 32] += a_s[r : r + 32, cols].astype(jnp.float32)

            wo_block(n).wait()

            @pl.when(jnp.logical_not(last & (theirs == 1)))
            def _():
                y_s[c] += _dot(seen_s[theirs], wo_s[slot], 1, 0)

            @pl.when(last & (theirs == 1))
            def _():
                a_s[:, cols] = (y_s[c] + _dot(seen_s[theirs], wo_s[slot], 1, 0)).astype(a_s.dtype)

            return 0

        lax.fori_loop(0, 2 * PARTS, block, 0)

    def fresh(st):
        top_s[st] = jnp.full(top_s.shape[1:], NEG, jnp.float32)
        mix_s[st] = jnp.zeros(mix_s.shape[1:], jnp.float32)

    def block(st, q, kv, b, which, masked):
        k, v = kv[0, b], kv[1, b]
        scores = [_dot(k, q[h, i], 1, 1) for h, i, _ in which]
        if masked:
            seen = lax.broadcasted_iota(jnp.int32, (T, T), 1) >= lax.broadcasted_iota(jnp.int32, (T, T), 0)
        weights_, keeps = [], []
        for (h, i, at), s in zip(which, scores):
            if (h, i) in masked:
                s = jnp.where(seen, s, HIDDEN)
            old = top_s[st, :, at : at + T]
            top = jnp.maximum(old, s.max(axis=0, keepdims=True))
            top_s[st, :, at : at + T] = top
            weights_.append(jnp.exp2((s - top) * e).astype(jnp.bfloat16))
            keeps.append(jnp.exp2((old - top) * e))
        values = jnp.concatenate([v.T, jnp.ones((8, T), jnp.bfloat16)], axis=0)
        for (h, i, at), p, keep in zip(which, weights_, keeps):
            mix_s[st, :, at : at + T] = mix_s[st, :, at : at + T] * keep + _dot(values, p, 1, 0)

    def whole(st, q, kv):
        lax.fori_loop(0, 2, lambda b, _: (block(st, q, kv, b, pieces, ()), 0)[1], 0)

    def diagonal(st, q, kv):
        block(st, q, kv, 0, pieces, ((0, 0), (1, 0)))
        block(st, q, kv, 1, [p for p in pieces if p[1] == 1], ((0, 1), (1, 1)))

    def finish(st, out, lse=None, given=None, given_lse=None, halves=(0, 1)):
        for h, i in [(h, i) for i in halves for h in range(2)]:
            at = pl.multiple_of((2 * h + i) * T, T)
            at = pl.ds(at, T)
            top, total = top_s[st, :, at] * scale, mix_s[st, HEAD : HEAD + 1, at]
            mix = mix_s[st, :HEAD, at]
            if given is None:
                mix = mix * (1 / total)
            else:
                before = given_lse[:, at]
                high = jnp.maximum(top, before)
                keep, add = jnp.exp(top - high), jnp.exp(before - high)
                top, total = high, total * keep + add
                mix = mix * (keep / total) + given[h, i].astype(jnp.float32).T * (add / total)
            out[h, i] = mix.T.astype(out.dtype)
            if lse is not None:
                lse[:, at] = top + jnp.log(total)

    spare = rounds

    def finish_b(d, j, out, lse=None, halves=(0, 1)):
        @pl.when(z > 0)
        def _():
            finish(spare, out, lse, part.at[d, j], part_lse.at[d, j], halves)

        @pl.when(z == 0)
        def _():
            finish(spare, out, lse, halves=halves)

    def arrived_b(d, j):
        @pl.when(z > 0)
        def _():
            p_arrived(d, j)

    barrier = pltpu.get_barrier_semaphore()
    for n in range(1, 2 * chips):
        pl.semaphore_signal(barrier, inc=1, device_id={"sp": lax.rem(me + n, 2 * chips)}, device_id_type=MESH)
    cuts = x_sem.shape[0]
    height = T // cuts

    def x_cut(i):
        rows = pl.ds(pl.multiple_of(i * height, height), height)
        return pltpu.make_async_copy(x_ref.at[rows], a_s.at[rows], x_sem.at[i])

    for i in range(cuts):
        x_cut(i).start()
    turns = pltpu.make_async_copy(turn_ref, turn_s, turn_sem.at[0])
    turns.start()
    group = min(64, height)
    tiles = [slice(c, c + HEAD) for c in range(0, D, HEAD)]

    def norm(i, _):
        x_cut(i).wait()

        @pl.when(i == 0)
        def _():
            weights(jnp.int32(0))

        def rows_(g, _):
            rows = pl.ds(pl.multiple_of(i * height + g * group, group), group)
            squares = jnp.zeros((group, HEAD), jnp.float32)
            for t in tiles:
                wide = a_s[rows, t].astype(jnp.float32)
                squares += wide * wide
            by = lax.rsqrt(squares.sum(axis=1, keepdims=True) / D + 1e-6)
            for n, t in enumerate(tiles):
                a_s[rows, t] = (a_s[rows, t].astype(jnp.float32) * by * gain_ref[n : n + 1].astype(jnp.float32)).astype(jnp.bfloat16)
            return 0

        return lax.fori_loop(0, height // group, rows_, 0)

    lax.fori_loop(0, cuts, norm, 0)
    base = (me * T).astype(jnp.float32) * speed_ref[...]
    side = jnp.where(lax.broadcasted_iota(jnp.int32, (1, HEAD), 1) < HEAD // 2, -1.0, 1.0)
    cos, sin = jnp.cos(base), jnp.sin(base)
    turns.wait()
    for r in range(0, T, 128):
        c, s_ = turn_s[0, r : r + 128], turn_s[1, r : r + 128]
        turn_s[0, r : r + 128] = c * cos - s_ * sin
        turn_s[1, r : r + 128] = s_ * (cos * side) + c * (sin * side)
    for n in range(WO_SLOTS - 1):
        wo_block(jnp.int32(n)).start()
    pl.semaphore_wait(barrier, 2 * chips - 1)

    def step(n, counts):
        projected, summed = counts
        code = task_at(n)
        kind, j, which = code & 15, lax.shift_right_logical(code, 4) & 3, lax.shift_right_logical(code, 6)

        @pl.when(kind == PROJECT)
        def _():
            project(j, which, projected)

        @pl.when(kind == KV_ON)
        def _():
            kv_arrived(which, j)
            kv_next(which, j).start()

        @pl.when(kind == Q_ON)
        def _():
            q_arrived(which, j)
            q_next(which, j).start()

        @pl.when(kind == A_OWN)
        def _():
            dd(0, 0, j).wait_recv()
            dd(0, 1, j).wait_recv()
            fresh(j)
            diagonal(j, own.at[0, 1, j], own.at[0, 0, j])

        @pl.when(kind == A_BELOW)
        def _():
            @pl.when(z == far)
            def _():
                kv_arrived(which, j)

            whole(j, own.at[0, 1, j], pool.at[which - 1, j])

        @pl.when(kind == A_END)
        def _():
            finish(j, own.at[0, 1, j])
            o_to(0, j).start()

        @pl.when(kind == B_KEYS)
        def _():
            dd(1, 0, j).wait_recv()

        @pl.when(kind == B_ABOVE)
        def _():
            @pl.when(z == 0)
            def _():
                q_arrived(which, j)

            fresh(spare)
            whole(spare, pool.at[far - which, j], own.at[1, 0, j])
            arrived_b(which, j)
            finish_b(which, j, part.at[held(which), j], lse_s.at[which - 1, j])
            p_to(which, j).start()
            l_to(which, j).start()

        @pl.when(kind == B_OWN)
        def _():
            dd(1, 1, j).wait_recv()
            fresh(spare)
            diagonal(spare, own.at[1, 1, j], own.at[1, 0, j])

            @pl.when(z > 0)
            def _():
                q_first(j, 0).wait_send()

            arrived_b(0, j)
            finish_b(0, j, own.at[1, 1, j], halves=(other,))
            o_to(1, j).start()
            finish_b(0, j, own.at[1, 1, j], halves=(core,))

        @pl.when(kind == SUM)
        def _():
            output(j, which, summed)

        return projected + jnp.where(kind == PROJECT, 1, 0), summed + jnp.where(kind == SUM, 1, 0)

    lax.fori_loop(0, STEPS, step, (jnp.int32(0), jnp.int32(0)))

    def drain(j, _):
        for ab in range(2):
            for isq in range(2):
                dd(ab, isq, j).wait_send()
            o_to(ab, j).wait_send()

        @pl.when(z < far)
        def _():
            for k in range(2):
                kv_first(j, k, 0).wait_send()
                kv_first(j, k, 1).wait_send()

        @pl.when(z > 0)
        def _():
            q_first(j, 1).wait_send()

        for s in range(1, far):

            @pl.when((z < far) & (s <= z))
            def _():
                kv_next(s, j).wait_send()

        for d in range(1, far):

            @pl.when((z > 0) & (d <= far - z))
            def _():
                q_next(d, j).wait_send()

        for d in range(1, chips):

            @pl.when(d <= far - z)
            def _():
                p_to(d, j).wait_send()
                l_to(d, j).wait_send()

        return 0

    lax.fori_loop(0, rounds, drain, 0)


def layer(x, gain, wq, wk, wv, wo, group):
    T, D, chips = *x.shape, group // 2
    rounds = wk.shape[1] // HEAD // 4
    low, wide = jnp.bfloat16, jnp.float32
    R, C = rounds, chips - 1
    dma = pltpu.SemaphoreType.DMA
    vmem, any_ = pl.BlockSpec(memory_space=pltpu.VMEM), pl.BlockSpec(memory_space=pl.ANY)
    weights = wq.size + wk.size + wv.size + wo.size
    speed = np.float32(THETA) ** (-np.arange(HEAD // 2, dtype=np.float32) / (HEAD // 2))
    angle = np.arange(T)[:, None] * np.concatenate([speed, speed]).astype(np.float64)
    turns = np.stack([np.cos(angle), np.sin(angle)]).astype(np.float32)
    return pl.pallas_call(
        functools.partial(_kernel, rounds, chips),
        out_shape=pltpu.VMEM((T, D), low),
        in_specs=[any_, vmem, vmem, any_, any_, any_, any_, any_],
        out_specs=vmem,
        scratch_shapes=[
            pltpu.VMEM((2, T, HEAD), wide),
            pltpu.VMEM((2, D, COLS), low),
            pltpu.VMEM((WO_SLOTS, 2 * HEAD, D // PARTS), low),
            pltpu.VMEM((2, T, 2 * HEAD), low),
            pltpu.VMEM((2, 2, R, 2, 2, T, HEAD), low),
            pltpu.VMEM((2, 2, R, 2, T, HEAD), low),
            pltpu.VMEM((C, R, 2, 2, T, HEAD), low),
            pltpu.VMEM((C, R, 2, 2, T, HEAD), low),
            pltpu.VMEM((C, R, 1, 4 * T), wide),
            pltpu.VMEM((C, R, 1, 4 * T), wide),
            pltpu.VMEM((2, R, 2, T, HEAD), low),
            pltpu.VMEM((R + 1, 1, 4 * T), wide),
            pltpu.VMEM((R + 1, HEAD + 8, 4 * T), wide),
            pltpu.VMEM((PARTS, T, D // PARTS), wide),
            dma((4,)), dma((1,)), dma((2,)), dma((WO_SLOTS,)),
            dma((2, 2, R)), dma((2, 2, R)),
            dma((2, 2, R)), dma((2, 2, R)),
            dma((C - 1, R)), dma((C - 1, R)),
            dma((2, R)), dma((2, R)),
            dma((C - 1, R)), dma((C - 1, R)),
            dma((C, R)), dma((C, R)),
            dma((C, R)), dma((C, R)),
            dma((2, R)), dma((2, R)),
        ],
        compiler_params=pltpu.CompilerParams(collective_id=0, has_side_effects=True, vmem_limit_bytes=VMEM),
        cost_estimate=pl.CostEstimate(flops=2 * T * weights + 8 * T * T * wq.shape[1], transcendentals=0, bytes_accessed=2 * weights),
    )(x, gain.reshape(D // HEAD, HEAD), np.concatenate([speed, speed])[None], turns, wq, wk, wv, wo)


def solution(mesh):
    group = mesh.shape["sp"]

    def step(x, gain, wq, wk, wv, wo):
        return layer(x, gain, wq, wk, wv, wo, group)

    tokens, whole = P(("dp", "sp"), None), P(None, None)
    return jax.shard_map(
        step,
        mesh=mesh,
        in_specs=(tokens, P(None), whole, whole, whole, whole),
        out_specs=tokens,
        check_vma=False,
    )
```

```python
import functools

import jax
import jax.numpy as jnp
import numpy as np
from jax import lax
from jax.experimental import pallas as pl
from jax.experimental.pallas import tpu as pltpu
from jax.sharding import PartitionSpec as P

STEPS = 64
TASKS = (
    (3178512, 9457664, 1656329, 2146327, 499776, 15771177, 2606688, 6829363, 4763798, 3698902, 6685670, 16136536, 581637, 11937059, 8835112, 1381175, 1595000, 658038, 657930, 657930, 657930, 10,),
    (1064960, 3166560, 7458944, 10511024, 14696944, 2110338, 2314868, 3706933, 9593953, 2670629, 10642985, 607235, 1246598, 545970, 7493145, 1574677, 4363848, 10907728, 3762215, 4617910, 3627031, 120,),
    (2101248, 10502496, 11591746, 3166289, 9551954, 6431632, 7459056, 7500851, 11841904, 3686453, 5510017, 202132, 4482145, 10584088, 8660388, 2688296, 6817831, 1656329, 5658647, 7747942, 489527, 72,),
    (13676608, 20672, 1077344, 14741632, 5510032, 4457376, 2109588, 6562692, 1430579, 11802740, 3683828, 525764, 2483364, 461096, 1513800, 2566488, 3619176, 658040, 657930, 657930, 657930, 10,),
)
PAIRS = (
    (6622244, 10461571, 31710,),
    (2921488, 9173735, 54582,),
    (12228672, 16137310, 8663,),
    (341985, 12526809, 36006,),
)
SUMS = (
    (4000486,),
    (16204307,),
    (10412171,),
    (16434201,),
)

PROJECT, KV_ON, Q_ON, A_OWN, A_BELOW, A_END, B_ABOVE, B_OWN, SUM, B_KEYS = range(10)

HEAD = 128
THETA = 10000
NEG = -1e30
HIDDEN = 2 * NEG
LOG2E = 1.4426950408889634
MESH = pl.DeviceIdType.MESH
COLS = 256
PARTS = 3
VMEM = 61_440_000


def _dot(a, b, ca, cb):
    return lax.dot_general(a, b, (((ca,), (cb,)), ((), ())), preferred_element_type=jnp.float32)


def _kernel(rounds, chips, x_ref, gain_ref, speed_ref, turn_ref, wq_ref, wk_ref, wv_ref, wo_ref, a_s, turn_s, w_s, wo_s, seen_s, own, staged, pool,
            part, part_lse, lse_s, o_got, top_s, mix_s, y_s, x_sem, turn_sem, w_sem, wo_sem, dd_send, dd_recv, kv_send, kv_recv, kvf_send,
            kvf_recv, q_send, q_recv, qf_send, qf_recv, p_send, p_recv, l_send, l_recv, o_send, o_recv):
    me = lax.axis_index("sp")
    z, core = lax.div(me, 2), lax.rem(me, 2)
    other = 1 - core
    mate = 2 * z + other
    above, below = lax.min(z + 1, chips - 1), lax.max(z - 1, 0)
    T, D = a_s.shape
    scale = HEAD**-0.5
    e = scale * LOG2E
    far = chips - 1
    pieces = [(h, i, (2 * h + i) * T) for h in range(2) for i in range(2)]

    def table(rows, per, bits):
        words = []
        for column in zip(*rows):
            w = jnp.int32(column[0])
            for c in range(1, chips):
                w = jnp.where(z == c, jnp.int32(column[c]), w)
            words.append(w)

        def entry(n):
            at = lax.div(n, per)
            w = words[0]
            for i in range(1, len(words)):
                w = jnp.where(at == i, words[i], w)
            return lax.shift_right_logical(w, bits * (n - per * at)) & (2**bits - 1)

        return entry

    task_at, pair_at, sum_at = table(TASKS, 3, 8), table(PAIRS, 6, 4), table(SUMS, 8, 3)

    def copy(src, dst, send, recv, to):
        return pltpu.make_async_remote_copy(src_ref=src, dst_ref=dst, send_sem=send, recv_sem=recv, device_id={"sp": to}, device_id_type=MESH)

    def dd(ab, isq, j):
        return copy(staged.at[ab, isq, j], own.at[ab, isq, j, :, core], dd_send.at[0], dd_recv.at[jnp.where(ab == 0, 0, 1 + isq), j], mate)

    def kv_first(j, k, theirs):
        src = staged.at[0, 0, j, k] if theirs else own.at[0, 0, j, k, core]
        to = 2 * above + (other if theirs else core)
        return copy(src, pool.at[0, j, k, core], kv_send.at[0], kv_recv.at[j], to)

    def kv_next(s, j):
        return copy(pool.at[s - 1, j], pool.at[s, j], kvf_send.at[0], kvf_recv.at[s - 1, j], 2 * above + core)

    def q_first(j, theirs):
        src = staged.at[1, 1, j] if theirs else own.at[1, 1, j, :, core]
        return copy(src, pool.at[far - 1, j, :, core], (q_send.at[rounds] if theirs else q_send.at[j]), q_recv.at[j], 2 * below + (other if theirs else core))

    def q_next(d, j):
        return copy(pool.at[far - d, j], pool.at[far - d - 1, j], qf_send.at[0], qf_recv.at[d - 1, j], 2 * below + core)

    def held(d):
        return jnp.where(z > 0, d, d - 1)

    def p_to(d, j):
        return copy(part.at[held(d), j], part.at[d - 1, j], p_send.at[0], p_recv.at[d - 1, j], 2 * above + core)

    def l_to(d, j):
        return copy(lse_s.at[d - 1, j], part_lse.at[d - 1, j], l_send.at[0], l_recv.at[d - 1, j], 2 * above + core)

    def o_to(ab, j):
        return copy(own.at[ab, 1, j, :, other], o_got.at[ab, j], o_send.at[0], o_recv.at[ab, j], mate)

    def arrived(ref, sem):
        copy(ref, ref, sem, sem, mate).wait_recv()

    def kv_arrived(s, j):
        @pl.when(s == 1)
        def _():
            arrived(pool.at[0, j], kv_recv.at[j])

        @pl.when(s > 1)
        def _():
            arrived(pool.at[s - 1, j], kvf_recv.at[s - 2, j])

    def q_arrived(d, j):
        @pl.when(d == 1)
        def _():
            arrived(pool.at[far - 1, j], q_recv.at[j])

        @pl.when(d > 1)
        def _():
            arrived(pool.at[far - d, j], qf_recv.at[d - 2, j])

    def p_arrived(d, j):
        arrived(part.at[d, j], p_recv.at[d, j])
        arrived(part_lse.at[d, j], l_recv.at[d, j])

    def weights(n):
        code = pair_at(lax.div(n, 2))
        j, pair, k = lax.div(code, 4), lax.rem(code, 4), lax.rem(n, 2)
        ab = jnp.where((pair == 1) | (pair == 2), 1, 0)
        at_kv = pl.ds(pl.multiple_of(COLS * (rounds * ab + j), COLS), COLS)
        at_q = pl.ds(pl.multiple_of(COLS * (2 * (rounds * ab + j) + k), COLS), COLS)
        isq = lax.rem(pair, 2)
        slot = lax.rem(n, 2)

        @pl.when((isq == 0) & (k == 0))
        def _():
            pltpu.make_async_copy(wk_ref.at[:, at_kv], w_s.at[slot], w_sem.at[slot]).start()

        @pl.when((isq == 0) & (k == 1))
        def _():
            pltpu.make_async_copy(wv_ref.at[:, at_kv], w_s.at[slot], w_sem.at[slot]).start()

        @pl.when(isq == 1)
        def _():
            pltpu.make_async_copy(wq_ref.at[:, at_q], w_s.at[slot], w_sem.at[slot]).start()

    def project(j, pair, done):
        isq = lax.rem(pair, 2)
        ab = jnp.where((pair == 1) | (pair == 2), 1, 0)

        def block(k, _):
            n = 2 * done + k
            slot = lax.rem(n, 2)

            @pl.when((n > 0) & (n + 1 < 8 * rounds))
            def _():
                weights(n + 1)

            pltpu.make_async_copy(wk_ref.at[:, pl.ds(0, COLS)], w_s.at[slot], w_sem.at[slot]).wait()
            turn = (isq == 1) | (k == 0)

            def head(t, u):
                plain = t.astype(jnp.bfloat16)
                f = plain.astype(jnp.float32)
                rotated = (f * turn_s[0] + pltpu.roll(f, HEAD // 2, 1) * turn_s[1]).astype(jnp.bfloat16)
                tile = jnp.where(turn, rotated, plain)
                owner = jnp.where(isq == 1, k, u)
                index = jnp.where(isq == 1, u, k)
                up = (pair == 0) & (z < far)

                @pl.when(owner == core)
                def _():
                    own[ab, isq, j, index, core] = tile

                    @pl.when(up)
                    def _():
                        kv_first(j, k, 0).start()

                @pl.when(owner != core)
                def _():
                    staged[ab, isq, j, index] = tile

                    @pl.when(up)
                    def _():
                        kv_first(j, k, 1).start()

            t = _dot(a_s[...], w_s[slot], 1, 0)
            for u in range(2):
                head(t[:, u * HEAD : (u + 1) * HEAD], u)

            return 0

        lax.fori_loop(0, 2, block, 0)

        @pl.when((pair == 1) & (z > 0))
        def _():
            q_first(j, 0).start()
            q_first(j, 1).start()

        dd(ab, isq, j).start()

        @pl.when(done == 4 * rounds - 1)
        def _():
            pltpu.make_async_copy(x_ref, a_s, x_sem.at[0]).start()

    def wo_block(n):
        who = jnp.where(lax.rem(n, 2) == 1, other, core)
        rows = pl.ds(pl.multiple_of(2 * HEAD * (2 * sum_at(lax.div(n, 2)) + who), 2 * HEAD), 2 * HEAD)
        slot = lax.rem(n, 2)
        return pltpu.make_async_copy(wo_ref.at[rows], wo_s.at[slot], wo_sem.at[slot])

    def output(j, ab, done):
        columns = [slice(c * (D // PARTS), (c + 1) * (D // PARTS)) for c in range(PARTS)]
        last = done == 2 * rounds - 1

        @pl.when(done == 0)
        def _():
            y_s[...] = jnp.zeros(y_s.shape, jnp.float32)

        @pl.when(done == 2 * rounds - 2)
        def _():
            pltpu.make_async_copy(x_ref, a_s, x_sem.at[0]).wait()

            def add(r, _):
                rows = pl.ds(pl.multiple_of(r * 32, 32), 32)
                y_s[rows, :] += a_s[rows, :].astype(jnp.float32)
                return 0

            lax.fori_loop(0, T // 32, add, 0)

        seen_s[...] = jnp.concatenate([own[ab, 1, j, 0, core], own[ab, 1, j, 1, core]], axis=1)

        def half(theirs, _):
            n = 2 * done + theirs

            @pl.when(n + 1 < 2 * 2 * rounds)
            def _():
                wo_block(n + 1).start()

            @pl.when(theirs == 1)
            def _():
                o_to(ab, j).wait_recv()
                seen_s[...] = jnp.concatenate([o_got[ab, j, 0], o_got[ab, j, 1]], axis=1)

            wo_block(n).wait()

            @pl.when(jnp.logical_not(last & (theirs == 1)))
            def _():
                for cols in columns:
                    y_s[:, cols] += _dot(seen_s[...], wo_s[theirs, :, cols], 1, 0)

            @pl.when(last & (theirs == 1))
            def _():
                for cols in columns:
                    a_s[:, cols] = (y_s[:, cols] + _dot(seen_s[...], wo_s[theirs, :, cols], 1, 0)).astype(a_s.dtype)

            return 0

        lax.fori_loop(0, 2, half, 0)

    def fresh(st):
        top_s[st] = jnp.full(top_s.shape[1:], NEG, jnp.float32)
        mix_s[st] = jnp.zeros(mix_s.shape[1:], jnp.float32)

    def block(st, q, kv, b, which, masked):
        k, v = kv[0, b], kv[1, b]
        scores = [_dot(k, q[h, i], 1, 1) for h, i, _ in which]
        if masked:
            seen = lax.broadcasted_iota(jnp.int32, (T, T), 1) >= lax.broadcasted_iota(jnp.int32, (T, T), 0)
        weights_, keeps = [], []
        for (h, i, at), s in zip(which, scores):
            if (h, i) in masked:
                s = jnp.where(seen, s, HIDDEN)
            old = top_s[st, :, at : at + T]
            top = jnp.maximum(old, s.max(axis=0, keepdims=True))
            top_s[st, :, at : at + T] = top
            weights_.append(jnp.exp2((s - top) * e).astype(jnp.bfloat16))
            keeps.append(jnp.exp2((old - top) * e))
        values = jnp.concatenate([v.T, jnp.ones((8, T), jnp.bfloat16)], axis=0)
        for (h, i, at), p, keep in zip(which, weights_, keeps):
            mix_s[st, :, at : at + T] = mix_s[st, :, at : at + T] * keep + _dot(values, p, 1, 0)

    def whole(st, q, kv):
        lax.fori_loop(0, 2, lambda b, _: (block(st, q, kv, b, pieces, ()), 0)[1], 0)

    def diagonal(st, q, kv):
        block(st, q, kv, 0, pieces, ((0, 0), (1, 0)))
        block(st, q, kv, 1, [p for p in pieces if p[1] == 1], ((0, 1), (1, 1)))

    def finish(st, out, lse=None, given=None, given_lse=None, halves=(0, 1)):
        for h, i in [(h, i) for i in halves for h in range(2)]:
            at = pl.multiple_of((2 * h + i) * T, T)
            at = pl.ds(at, T)
            top, total = top_s[st, :, at] * scale, mix_s[st, HEAD : HEAD + 1, at]
            mix = mix_s[st, :HEAD, at]
            if given is None:
                mix = mix * (1 / total)
            else:
                before = given_lse[:, at]
                high = jnp.maximum(top, before)
                keep, add = jnp.exp(top - high), jnp.exp(before - high)
                top, total = high, total * keep + add
                mix = mix * (keep / total) + given[h, i].astype(jnp.float32).T * (add / total)
            out[h, i] = mix.T.astype(out.dtype)
            if lse is not None:
                lse[:, at] = top + jnp.log(total)

    spare = rounds

    def finish_b(d, j, out, lse=None, halves=(0, 1)):
        @pl.when(z > 0)
        def _():
            finish(spare, out, lse, part.at[d, j], part_lse.at[d, j], halves)

        @pl.when(z == 0)
        def _():
            finish(spare, out, lse, halves=halves)

    def arrived_b(d, j):
        @pl.when(z > 0)
        def _():
            p_arrived(d, j)

    barrier = pltpu.get_barrier_semaphore()
    for n in range(1, 2 * chips):
        pl.semaphore_signal(barrier, inc=1, device_id={"sp": lax.rem(me + n, 2 * chips)}, device_id_type=MESH)
    cuts = x_sem.shape[0]
    height = T // cuts

    def x_cut(i):
        rows = pl.ds(pl.multiple_of(i * height, height), height)
        return pltpu.make_async_copy(x_ref.at[rows], a_s.at[rows], x_sem.at[i])

    for i in range(cuts):
        x_cut(i).start()
    turns = pltpu.make_async_copy(turn_ref, turn_s, turn_sem.at[0])
    turns.start()
    tiles = [slice(c, c + HEAD) for c in range(0, D, HEAD)]

    def norm(i, _):
        x_cut(i).wait()

        @pl.when(i == cuts // 2)
        def _():
            weights(jnp.int32(0))

        rows = pl.ds(pl.multiple_of(i * height, height), height)
        squares = jnp.zeros((height, HEAD), jnp.float32)
        for t in tiles:
            wide = a_s[rows, t].astype(jnp.float32)
            squares += wide * wide
        by = lax.rsqrt(squares.sum(axis=1, keepdims=True) / D + 1e-6)
        for n, t in enumerate(tiles):
            a_s[rows, t] = (a_s[rows, t].astype(jnp.float32) * by * gain_ref[n : n + 1].astype(jnp.float32)).astype(jnp.bfloat16)
        return 0

    lax.fori_loop(0, cuts, norm, 0)
    weights(jnp.int32(1))
    base = (me * T).astype(jnp.float32) * speed_ref[...]
    side = jnp.where(lax.broadcasted_iota(jnp.int32, (1, HEAD), 1) < HEAD // 2, -1.0, 1.0)
    cos, sin = jnp.cos(base), jnp.sin(base)
    turns.wait()
    for r in range(0, T, 128):
        c, s_ = turn_s[0, r : r + 128], turn_s[1, r : r + 128]
        turn_s[0, r : r + 128] = c * cos - s_ * sin
        turn_s[1, r : r + 128] = s_ * (cos * side) + c * (sin * side)
    wo_block(jnp.int32(0)).start()
    pl.semaphore_wait(barrier, 2 * chips - 1)

    def step(n, counts):
        projected, summed = counts
        code = task_at(n)
        kind, j, which = code & 15, lax.shift_right_logical(code, 4) & 3, lax.shift_right_logical(code, 6)

        @pl.when(kind == PROJECT)
        def _():
            project(j, which, projected)

        @pl.when(kind == KV_ON)
        def _():
            kv_arrived(which, j)
            kv_next(which, j).start()

        @pl.when(kind == Q_ON)
        def _():
            q_arrived(which, j)
            q_next(which, j).start()

        @pl.when(kind == A_OWN)
        def _():
            arrived(own.at[0, :, j, :, other], dd_recv.at[0, j])
            fresh(j)
            diagonal(j, own.at[0, 1, j], own.at[0, 0, j])

        @pl.when(kind == A_BELOW)
        def _():
            @pl.when(z == far)
            def _():
                kv_arrived(which, j)

            whole(j, own.at[0, 1, j], pool.at[which - 1, j])

        @pl.when(kind == A_END)
        def _():
            finish(j, own.at[0, 1, j])
            o_to(0, j).start()

        @pl.when(kind == B_KEYS)
        def _():
            arrived(own.at[1, 0, j, :, other], dd_recv.at[1, j])

        @pl.when(kind == B_ABOVE)
        def _():
            @pl.when(z == 0)
            def _():
                q_arrived(which, j)

            fresh(spare)
            whole(spare, pool.at[far - which, j], own.at[1, 0, j])
            arrived_b(which, j)
            finish_b(which, j, part.at[held(which), j], lse_s.at[which - 1, j])
            p_to(which, j).start()
            l_to(which, j).start()

        @pl.when(kind == B_OWN)
        def _():
            arrived(own.at[1, 1, j, :, other], dd_recv.at[2, j])
            fresh(spare)
            diagonal(spare, own.at[1, 1, j], own.at[1, 0, j])

            @pl.when(z > 0)
            def _():
                q_first(j, 0).wait_send()

            arrived_b(0, j)
            finish_b(0, j, own.at[1, 1, j], halves=(other,))
            o_to(1, j).start()
            finish_b(0, j, own.at[1, 1, j], halves=(core,))

        @pl.when(kind == SUM)
        def _():
            output(j, which, summed)

        return projected + jnp.where(kind == PROJECT, 1, 0), summed + jnp.where(kind == SUM, 1, 0)

    lax.fori_loop(0, STEPS, step, (jnp.int32(0), jnp.int32(0)))

    def sent(ref, sem):
        copy(ref, ref, sem, sem, mate).wait_send()

    def drain():
        sent(staged, dd_send.at[0])
        sent(o_got, o_send.at[0])

        @pl.when(z < far)
        def _():
            sent(staged.at[0], kv_send.at[0])

        @pl.when(z > 0)
        def _():
            sent(staged.at[1, 1], q_send.at[rounds])

        for c in range(chips):

            @pl.when(z == c)
            def _():
                if 0 < c < far:
                    sent(pool.at[pl.ds(0, c)], kvf_send.at[0])
                    sent(pool.at[pl.ds(0, far - c)], qf_send.at[0])
                if c < far:
                    sent(part.at[pl.ds(0, far - c)], p_send.at[0])
                    sent(part_lse.at[pl.ds(0, far - c)], l_send.at[0])

    drain()


def layer(x, gain, wq, wk, wv, wo, group):
    T, D, chips = *x.shape, group // 2
    rounds = wk.shape[1] // HEAD // 4
    low, wide = jnp.bfloat16, jnp.float32
    R, C = rounds, chips - 1
    dma = pltpu.SemaphoreType.DMA
    vmem, any_ = pl.BlockSpec(memory_space=pltpu.VMEM), pl.BlockSpec(memory_space=pl.ANY)
    weights = wq.size + wk.size + wv.size + wo.size
    speed = np.float32(THETA) ** (-np.arange(HEAD // 2, dtype=np.float32) / (HEAD // 2))
    angle = np.arange(T)[:, None] * np.concatenate([speed, speed]).astype(np.float64)
    turns = np.stack([np.cos(angle), np.sin(angle)]).astype(np.float32)
    return pl.pallas_call(
        functools.partial(_kernel, rounds, chips),
        out_shape=pltpu.VMEM((T, D), low),
        in_specs=[any_, vmem, vmem, any_, any_, any_, any_, any_],
        out_specs=vmem,
        scratch_shapes=[
            pltpu.VMEM((2, T, HEAD), wide),
            pltpu.VMEM((2, D, COLS), low),
            pltpu.VMEM((2, 2 * HEAD, D), low),
            pltpu.VMEM((T, 2 * HEAD), low),
            pltpu.VMEM((2, 2, R, 2, 2, T, HEAD), low),
            pltpu.VMEM((2, 2, R, 2, T, HEAD), low),
            pltpu.VMEM((C, R, 2, 2, T, HEAD), low),
            pltpu.VMEM((C, R, 2, 2, T, HEAD), low),
            pltpu.VMEM((C, R, 1, 4 * T), wide),
            pltpu.VMEM((C, R, 1, 4 * T), wide),
            pltpu.VMEM((2, R, 2, T, HEAD), low),
            pltpu.VMEM((R + 1, 1, 4 * T), wide),
            pltpu.VMEM((R + 1, HEAD + 8, 4 * T), wide),
            pltpu.VMEM((T, D), wide),
            dma((8,)), dma((1,)), dma((2,)), dma((2,)),
            dma((1,)), dma((3, R)),
            dma((1,)), dma((R,)),
            dma((1,)), dma((C - 1, R)),
            dma((R + 1,)), dma((R,)),
            dma((1,)), dma((C - 1, R)),
            dma((1,)), dma((C, R)),
            dma((1,)), dma((C, R)),
            dma((1,)), dma((2, R)),
        ],
        compiler_params=pltpu.CompilerParams(collective_id=0, has_side_effects=True, vmem_limit_bytes=VMEM),
        cost_estimate=pl.CostEstimate(flops=2 * T * weights + 8 * T * T * wq.shape[1], transcendentals=0, bytes_accessed=2 * weights),
    )(x, gain.reshape(D // HEAD, HEAD), np.concatenate([speed, speed])[None], turns, wq, wk, wv, wo)


def solution(mesh):
    group = mesh.shape["sp"]

    def step(x, gain, wq, wk, wv, wo):
        return layer(x, gain, wq, wk, wv, wo, group)

    tokens, whole = P(("dp", "sp"), None), P(None, None)
    return jax.shard_map(
        step,
        mesh=mesh,
        in_specs=(tokens, P(None), whole, whole, whole, whole),
        out_specs=tokens,
        check_vma=False,
    )
```

```python
import functools

import jax
import jax.numpy as jnp
import numpy as np
from jax import lax
from jax.experimental import pallas as pl
from jax.experimental.pallas import tpu as pltpu
from jax.sharding import PartitionSpec as P

STEPS = 64
TASKS = (
    (3178512, 9457664, 1656329, 2146327, 499776, 15771177, 2606688, 6829363, 4763798, 3698902, 6685670, 16136536, 581637, 11937059, 8835112, 1381175, 1595000, 658038, 657930, 657930, 657930, 10,),
    (1064960, 3166560, 7458944, 10511024, 14696944, 2110338, 2314868, 3706933, 9593953, 2670629, 10642985, 607235, 1246598, 545970, 7493145, 1574677, 4363848, 10907728, 3762215, 4617910, 3627031, 120,),
    (2101248, 10502496, 11591746, 3166289, 9551954, 6431632, 7459056, 7500851, 11841904, 3686453, 5510017, 202132, 4482145, 10584088, 8660388, 2688296, 6817831, 1656329, 5658647, 7747942, 489527, 72,),
    (13676608, 20672, 1077344, 14741632, 5510032, 4457376, 2109588, 6562692, 1430579, 11802740, 3683828, 525764, 2483364, 461096, 1513800, 2566488, 3619176, 658040, 657930, 657930, 657930, 10,),
)
PAIRS = (
    (6622244, 10461571, 31710,),
    (2921488, 9173735, 54582,),
    (12228672, 16137310, 8663,),
    (341985, 12526809, 36006,),
)
SUMS = (
    (4000486,),
    (16204307,),
    (10412171,),
    (16434201,),
)

PROJECT, KV_ON, Q_ON, A_OWN, A_BELOW, A_END, B_ABOVE, B_OWN, SUM, B_KEYS = range(10)

HEAD = 128
THETA = 10000
NEG = -1e30
HIDDEN = 2 * NEG
LOG2E = 1.4426950408889634
MESH = pl.DeviceIdType.MESH
COLS = 256
PARTS = 3
VMEM = 61_440_000


def _dot(a, b, ca, cb):
    return lax.dot_general(a, b, (((ca,), (cb,)), ((), ())), preferred_element_type=jnp.float32)


def _kernel(rounds, chips, x_ref, gain_ref, speed_ref, turn_ref, wq_ref, wk_ref, wv_ref, wo_ref, a_s, turn_s, w_s, wo_s, seen_s, own, staged, pool,
            part, part_lse, lse_s, o_got, top_s, mix_s, y_s, x_sem, turn_sem, w_sem, wo_sem, dd_send, dd_recv, kv_send, kv_recv, kvf_send,
            kvf_recv, q_send, q_recv, qf_send, qf_recv, p_send, p_recv, l_send, l_recv, o_send, o_recv):
    me = lax.axis_index("sp")
    z, core = lax.div(me, 2), lax.rem(me, 2)
    other = 1 - core
    mate = 2 * z + other
    above, below = lax.min(z + 1, chips - 1), lax.max(z - 1, 0)
    T, D = a_s.shape
    scale = HEAD**-0.5
    e = scale * LOG2E
    far = chips - 1
    pieces = [(h, i, (2 * h + i) * T) for h in range(2) for i in range(2)]

    def table(rows, per, bits):
        words = []
        for column in zip(*rows):
            w = jnp.int32(column[0])
            for c in range(1, chips):
                w = jnp.where(z == c, jnp.int32(column[c]), w)
            words.append(w)

        def entry(n):
            at = lax.div(n, per)
            w = words[0]
            for i in range(1, len(words)):
                w = jnp.where(at == i, words[i], w)
            return lax.shift_right_logical(w, bits * (n - per * at)) & (2**bits - 1)

        return entry

    task_at, pair_at, sum_at = table(TASKS, 3, 8), table(PAIRS, 6, 4), table(SUMS, 8, 3)

    def copy(src, dst, send, recv, to):
        return pltpu.make_async_remote_copy(src_ref=src, dst_ref=dst, send_sem=send, recv_sem=recv, device_id={"sp": to}, device_id_type=MESH)

    def dd(ab, isq, j):
        return copy(staged.at[ab, isq, j], own.at[ab, isq, j, :, core], dd_send.at[0], dd_recv.at[jnp.where(ab == 0, 0, 1 + isq), j], mate)

    def kv_first(j, k, theirs):
        src = staged.at[0, 0, j, k] if theirs else own.at[0, 0, j, k, core]
        to = 2 * above + (other if theirs else core)
        return copy(src, pool.at[0, j, k, core], kv_send.at[0], kv_recv.at[j], to)

    def kv_next(s, j):
        return copy(pool.at[s - 1, j], pool.at[s, j], kvf_send.at[0], kvf_recv.at[s - 1, j], 2 * above + core)

    def q_first(j, theirs):
        src = staged.at[1, 1, j] if theirs else own.at[1, 1, j, :, core]
        return copy(src, pool.at[far - 1, j, :, core], (q_send.at[rounds] if theirs else q_send.at[j]), q_recv.at[j], 2 * below + (other if theirs else core))

    def q_next(d, j):
        return copy(pool.at[far - d, j], pool.at[far - d - 1, j], qf_send.at[0], qf_recv.at[d - 1, j], 2 * below + core)

    def held(d):
        return jnp.where(z > 0, d, d - 1)

    def p_to(d, j):
        return copy(part.at[held(d), j], part.at[d - 1, j], p_send.at[0], p_recv.at[d - 1, j], 2 * above + core)

    def l_to(d, j):
        return copy(lse_s.at[d - 1, j], part_lse.at[d - 1, j], l_send.at[0], l_recv.at[d - 1, j], 2 * above + core)

    def o_to(ab, j):
        return copy(own.at[ab, 1, j, :, other], o_got.at[ab, j], o_send.at[0], o_recv.at[ab, j], mate)

    def arrived(ref, sem):
        copy(ref, ref, sem, sem, mate).wait_recv()

    def kv_arrived(s, j):
        @pl.when(s == 1)
        def _():
            arrived(pool.at[0, j], kv_recv.at[j])

        @pl.when(s > 1)
        def _():
            arrived(pool.at[s - 1, j], kvf_recv.at[s - 2, j])

    def q_arrived(d, j):
        @pl.when(d == 1)
        def _():
            arrived(pool.at[far - 1, j], q_recv.at[j])

        @pl.when(d > 1)
        def _():
            arrived(pool.at[far - d, j], qf_recv.at[d - 2, j])

    def p_arrived(d, j):
        arrived(part.at[d, j], p_recv.at[d, j])
        arrived(part_lse.at[d, j], l_recv.at[d, j])

    def weights(n):
        code = pair_at(lax.div(n, 2))
        j, pair, k = lax.div(code, 4), lax.rem(code, 4), lax.rem(n, 2)
        ab = jnp.where((pair == 1) | (pair == 2), 1, 0)
        at_kv = pl.ds(pl.multiple_of(COLS * (rounds * ab + j), COLS), COLS)
        at_q = pl.ds(pl.multiple_of(COLS * (2 * (rounds * ab + j) + k), COLS), COLS)
        isq = lax.rem(pair, 2)
        slot = lax.rem(n, 2)

        @pl.when((isq == 0) & (k == 0))
        def _():
            pltpu.make_async_copy(wk_ref.at[:, at_kv], w_s.at[slot], w_sem.at[slot]).start()

        @pl.when((isq == 0) & (k == 1))
        def _():
            pltpu.make_async_copy(wv_ref.at[:, at_kv], w_s.at[slot], w_sem.at[slot]).start()

        @pl.when(isq == 1)
        def _():
            pltpu.make_async_copy(wq_ref.at[:, at_q], w_s.at[slot], w_sem.at[slot]).start()

    def project(j, pair, done):
        isq = lax.rem(pair, 2)
        ab = jnp.where((pair == 1) | (pair == 2), 1, 0)

        def block(k, _):
            n = 2 * done + k
            slot = lax.rem(n, 2)

            @pl.when((n > 0) & (n + 1 < 8 * rounds))
            def _():
                weights(n + 1)

            pltpu.make_async_copy(wk_ref.at[:, pl.ds(0, COLS)], w_s.at[slot], w_sem.at[slot]).wait()
            turn = (isq == 1) | (k == 0)

            def head(t, u):
                plain = t.astype(jnp.bfloat16)
                f = plain.astype(jnp.float32)
                rotated = (f * turn_s[0] + pltpu.roll(f, HEAD // 2, 1) * turn_s[1]).astype(jnp.bfloat16)
                tile = jnp.where(turn, rotated, plain)
                owner = jnp.where(isq == 1, k, u)
                index = jnp.where(isq == 1, u, k)
                up = (pair == 0) & (z < far)

                @pl.when(owner == core)
                def _():
                    own[ab, isq, j, index, core] = tile

                    @pl.when(up)
                    def _():
                        kv_first(j, k, 0).start()

                @pl.when(owner != core)
                def _():
                    staged[ab, isq, j, index] = tile

                    @pl.when(up)
                    def _():
                        kv_first(j, k, 1).start()

            t = _dot(a_s[...], w_s[slot], 1, 0)
            for u in range(2):
                head(t[:, u * HEAD : (u + 1) * HEAD], u)

            return 0

        lax.fori_loop(0, 2, block, 0)

        @pl.when((pair == 1) & (z > 0))
        def _():
            q_first(j, 0).start()
            q_first(j, 1).start()

        dd(ab, isq, j).start()

        @pl.when(done == 4 * rounds - 1)
        def _():
            pltpu.make_async_copy(x_ref, a_s, x_sem.at[0]).start()

    def wo_block(n):
        who = jnp.where(lax.rem(n, 2) == 1, other, core)
        rows = pl.ds(pl.multiple_of(2 * HEAD * (2 * sum_at(lax.div(n, 2)) + who), 2 * HEAD), 2 * HEAD)
        slot = lax.rem(n, 2)
        return pltpu.make_async_copy(wo_ref.at[rows], wo_s.at[slot], wo_sem.at[slot])

    def output(j, ab, done):
        columns = [slice(c * (D // PARTS), (c + 1) * (D // PARTS)) for c in range(PARTS)]
        last = done == 2 * rounds - 1

        @pl.when(done == 0)
        def _():
            y_s[...] = jnp.zeros(y_s.shape, jnp.float32)

        @pl.when(done == 2 * rounds - 2)
        def _():
            pltpu.make_async_copy(x_ref, a_s, x_sem.at[0]).wait()

            def add(r, _):
                rows = pl.ds(pl.multiple_of(r * 32, 32), 32)
                y_s[rows, :] += a_s[rows, :].astype(jnp.float32)
                return 0

            lax.fori_loop(0, T // 32, add, 0)

        seen_s[...] = jnp.concatenate([own[ab, 1, j, 0, core], own[ab, 1, j, 1, core]], axis=1)

        def half(theirs, _):
            n = 2 * done + theirs

            @pl.when(n + 1 < 2 * 2 * rounds)
            def _():
                wo_block(n + 1).start()

            @pl.when(theirs == 1)
            def _():
                o_to(ab, j).wait_recv()
                seen_s[...] = jnp.concatenate([o_got[ab, j, 0], o_got[ab, j, 1]], axis=1)

            wo_block(n).wait()

            @pl.when(jnp.logical_not(last & (theirs == 1)))
            def _():
                for cols in columns:
                    y_s[:, cols] += _dot(seen_s[...], wo_s[theirs, :, cols], 1, 0)

            @pl.when(last & (theirs == 1))
            def _():
                for cols in columns:
                    a_s[:, cols] = (y_s[:, cols] + _dot(seen_s[...], wo_s[theirs, :, cols], 1, 0)).astype(a_s.dtype)

            return 0

        lax.fori_loop(0, 2, half, 0)

    def fresh(st):
        top_s[st] = jnp.full(top_s.shape[1:], NEG, jnp.float32)
        mix_s[st] = jnp.zeros(mix_s.shape[1:], jnp.float32)

    def block(st, q, kv, b, which, masked):
        k, v = kv[0, b], kv[1, b]
        scores = [_dot(k, q[h, i], 1, 1) for h, i, _ in which]
        if masked:
            seen = lax.broadcasted_iota(jnp.int32, (T, T), 1) >= lax.broadcasted_iota(jnp.int32, (T, T), 0)
        weights_, keeps = [], []
        for (h, i, at), s in zip(which, scores):
            if (h, i) in masked:
                s = jnp.where(seen, s, HIDDEN)
            old = top_s[st, :, at : at + T]
            top = jnp.maximum(old, s.max(axis=0, keepdims=True))
            top_s[st, :, at : at + T] = top
            weights_.append(jnp.exp2((s - top) * e).astype(jnp.bfloat16))
            keeps.append(jnp.exp2((old - top) * e))
        values = jnp.concatenate([v.T, jnp.ones((8, T), jnp.bfloat16)], axis=0)
        for (h, i, at), p, keep in zip(which, weights_, keeps):
            mix_s[st, :, at : at + T] = mix_s[st, :, at : at + T] * keep + _dot(values, p, 1, 0)

    def whole(st, q, kv):
        lax.fori_loop(0, 2, lambda b, _: (block(st, q, kv, b, pieces, ()), 0)[1], 0)

    def diagonal(st, q, kv):
        block(st, q, kv, 0, pieces, ((0, 0), (1, 0)))
        block(st, q, kv, 1, [p for p in pieces if p[1] == 1], ((0, 1), (1, 1)))

    def finish(st, out, lse=None, given=None, given_lse=None, halves=(0, 1)):
        for h, i in [(h, i) for i in halves for h in range(2)]:
            at = pl.multiple_of((2 * h + i) * T, T)
            at = pl.ds(at, T)
            top, total = top_s[st, :, at] * scale, mix_s[st, HEAD : HEAD + 1, at]
            mix = mix_s[st, :HEAD, at]
            if given is None:
                mix = mix * (1 / total)
            else:
                before = given_lse[:, at]
                high = jnp.maximum(top, before)
                keep, add = jnp.exp(top - high), jnp.exp(before - high)
                top, total = high, total * keep + add
                mix = mix * (keep / total) + given[h, i].astype(jnp.float32).T * (add / total)
            out[h, i] = mix.T.astype(out.dtype)
            if lse is not None:
                lse[:, at] = top + jnp.log(total)

    spare = rounds

    def finish_b(d, j, out, lse=None, halves=(0, 1)):
        @pl.when(z > 0)
        def _():
            finish(spare, out, lse, part.at[d, j], part_lse.at[d, j], halves)

        @pl.when(z == 0)
        def _():
            finish(spare, out, lse, halves=halves)

    def arrived_b(d, j):
        @pl.when(z > 0)
        def _():
            p_arrived(d, j)

    barrier = pltpu.get_barrier_semaphore()
    for n in range(1, 2 * chips):
        pl.semaphore_signal(barrier, inc=1, device_id={"sp": lax.rem(me + n, 2 * chips)}, device_id_type=MESH)
    cuts = x_sem.shape[0]
    height = T // cuts

    def x_cut(i):
        rows = pl.ds(pl.multiple_of(i * height, height), height)
        return pltpu.make_async_copy(x_ref.at[rows], a_s.at[rows], x_sem.at[i])

    for i in range(cuts):
        x_cut(i).start()
    turns = pltpu.make_async_copy(turn_ref, turn_s, turn_sem.at[0])
    turns.start()
    tiles = [slice(c, c + HEAD) for c in range(0, D, HEAD)]

    def norm(i, _):
        x_cut(i).wait()

        @pl.when(i == cuts // 4)
        def _():
            weights(jnp.int32(0))

        rows = pl.ds(pl.multiple_of(i * height, height), height)
        squares = jnp.zeros((height, HEAD), jnp.float32)
        for t in tiles:
            wide = a_s[rows, t].astype(jnp.float32)
            squares += wide * wide
        by = lax.rsqrt(squares.sum(axis=1, keepdims=True) / D + 1e-6)
        for n, t in enumerate(tiles):
            a_s[rows, t] = (a_s[rows, t].astype(jnp.float32) * by * gain_ref[n : n + 1].astype(jnp.float32)).astype(jnp.bfloat16)
        return 0

    lax.fori_loop(0, cuts, norm, 0)
    weights(jnp.int32(1))
    base = (me * T).astype(jnp.float32) * speed_ref[...]
    side = jnp.where(lax.broadcasted_iota(jnp.int32, (1, HEAD), 1) < HEAD // 2, -1.0, 1.0)
    cos, sin = jnp.cos(base), jnp.sin(base)
    turns.wait()
    for r in range(0, T, 128):
        c, s_ = turn_s[0, r : r + 128], turn_s[1, r : r + 128]
        turn_s[0, r : r + 128] = c * cos - s_ * sin
        turn_s[1, r : r + 128] = s_ * (cos * side) + c * (sin * side)
    wo_block(jnp.int32(0)).start()
    pl.semaphore_wait(barrier, 2 * chips - 1)

    def step(n, counts):
        projected, summed = counts
        code = task_at(n)
        kind, j, which = code & 15, lax.shift_right_logical(code, 4) & 3, lax.shift_right_logical(code, 6)

        @pl.when(kind == PROJECT)
        def _():
            project(j, which, projected)

        @pl.when(kind == KV_ON)
        def _():
            kv_arrived(which, j)
            kv_next(which, j).start()

        @pl.when(kind == Q_ON)
        def _():
            q_arrived(which, j)
            q_next(which, j).start()

        @pl.when(kind == A_OWN)
        def _():
            arrived(own.at[0, :, j, :, other], dd_recv.at[0, j])
            fresh(j)
            diagonal(j, own.at[0, 1, j], own.at[0, 0, j])

        @pl.when(kind == A_BELOW)
        def _():
            @pl.when(z == far)
            def _():
                kv_arrived(which, j)

            whole(j, own.at[0, 1, j], pool.at[which - 1, j])

        @pl.when(kind == A_END)
        def _():
            finish(j, own.at[0, 1, j])
            o_to(0, j).start()

        @pl.when(kind == B_KEYS)
        def _():
            arrived(own.at[1, 0, j, :, other], dd_recv.at[1, j])

        @pl.when(kind == B_ABOVE)
        def _():
            @pl.when(z == 0)
            def _():
                q_arrived(which, j)

            fresh(spare)
            whole(spare, pool.at[far - which, j], own.at[1, 0, j])
            arrived_b(which, j)
            finish_b(which, j, part.at[held(which), j], lse_s.at[which - 1, j])
            p_to(which, j).start()
            l_to(which, j).start()

        @pl.when(kind == B_OWN)
        def _():
            arrived(own.at[1, 1, j, :, other], dd_recv.at[2, j])
            fresh(spare)
            diagonal(spare, own.at[1, 1, j], own.at[1, 0, j])

            @pl.when(z > 0)
            def _():
                q_first(j, 0).wait_send()

            arrived_b(0, j)
            finish_b(0, j, own.at[1, 1, j], halves=(other,))
            o_to(1, j).start()
            finish_b(0, j, own.at[1, 1, j], halves=(core,))

        @pl.when(kind == SUM)
        def _():
            output(j, which, summed)

        return projected + jnp.where(kind == PROJECT, 1, 0), summed + jnp.where(kind == SUM, 1, 0)

    lax.fori_loop(0, STEPS, step, (jnp.int32(0), jnp.int32(0)))

    def sent(ref, sem):
        copy(ref, ref, sem, sem, mate).wait_send()

    def drain():
        sent(staged, dd_send.at[0])
        sent(o_got, o_send.at[0])

        @pl.when(z < far)
        def _():
            sent(staged.at[0], kv_send.at[0])

        @pl.when(z > 0)
        def _():
            sent(staged.at[1, 1], q_send.at[rounds])

        for c in range(chips):

            @pl.when(z == c)
            def _():
                if 0 < c < far:
                    sent(pool.at[pl.ds(0, c)], kvf_send.at[0])
                    sent(pool.at[pl.ds(0, far - c)], qf_send.at[0])
                if c < far:
                    sent(part.at[pl.ds(0, far - c)], p_send.at[0])
                    sent(part_lse.at[pl.ds(0, far - c)], l_send.at[0])

    drain()


def layer(x, gain, wq, wk, wv, wo, group):
    T, D, chips = *x.shape, group // 2
    rounds = wk.shape[1] // HEAD // 4
    low, wide = jnp.bfloat16, jnp.float32
    R, C = rounds, chips - 1
    dma = pltpu.SemaphoreType.DMA
    vmem, any_ = pl.BlockSpec(memory_space=pltpu.VMEM), pl.BlockSpec(memory_space=pl.ANY)
    weights = wq.size + wk.size + wv.size + wo.size
    speed = np.float32(THETA) ** (-np.arange(HEAD // 2, dtype=np.float32) / (HEAD // 2))
    angle = np.arange(T)[:, None] * np.concatenate([speed, speed]).astype(np.float64)
    turns = np.stack([np.cos(angle), np.sin(angle)]).astype(np.float32)
    return pl.pallas_call(
        functools.partial(_kernel, rounds, chips),
        out_shape=pltpu.VMEM((T, D), low),
        in_specs=[any_, vmem, vmem, any_, any_, any_, any_, any_],
        out_specs=vmem,
        scratch_shapes=[
            pltpu.VMEM((2, T, HEAD), wide),
            pltpu.VMEM((2, D, COLS), low),
            pltpu.VMEM((2, 2 * HEAD, D), low),
            pltpu.VMEM((T, 2 * HEAD), low),
            pltpu.VMEM((2, 2, R, 2, 2, T, HEAD), low),
            pltpu.VMEM((2, 2, R, 2, T, HEAD), low),
            pltpu.VMEM((C, R, 2, 2, T, HEAD), low),
            pltpu.VMEM((C, R, 2, 2, T, HEAD), low),
            pltpu.VMEM((C, R, 1, 4 * T), wide),
            pltpu.VMEM((C, R, 1, 4 * T), wide),
            pltpu.VMEM((2, R, 2, T, HEAD), low),
            pltpu.VMEM((R + 1, 1, 4 * T), wide),
            pltpu.VMEM((R + 1, HEAD + 8, 4 * T), wide),
            pltpu.VMEM((T, D), wide),
            dma((8,)), dma((1,)), dma((2,)), dma((2,)),
            dma((1,)), dma((3, R)),
            dma((1,)), dma((R,)),
            dma((1,)), dma((C - 1, R)),
            dma((R + 1,)), dma((R,)),
            dma((1,)), dma((C - 1, R)),
            dma((1,)), dma((C, R)),
            dma((1,)), dma((C, R)),
            dma((1,)), dma((2, R)),
        ],
        compiler_params=pltpu.CompilerParams(collective_id=0, has_side_effects=True, vmem_limit_bytes=VMEM),
        cost_estimate=pl.CostEstimate(flops=2 * T * weights + 8 * T * T * wq.shape[1], transcendentals=0, bytes_accessed=2 * weights),
    )(x, gain.reshape(D // HEAD, HEAD), np.concatenate([speed, speed])[None], turns, wq, wk, wv, wo)


def solution(mesh):
    group = mesh.shape["sp"]

    def step(x, gain, wq, wk, wv, wo):
        return layer(x, gain, wq, wk, wv, wo, group)

    tokens, whole = P(("dp", "sp"), None), P(None, None)
    return jax.shard_map(
        step,
        mesh=mesh,
        in_specs=(tokens, P(None), whole, whole, whole, whole),
        out_specs=tokens,
        check_vma=False,
    )
```
